32 devices in a mesh: freq: 8 (over z, y), rows: 4 (over x, core).
Axes of the slice: x: 2, y: 2, z: 4, core: 2. Of those that a mesh axis runs over, the one named last changes fastest.
Arguments:
- wavefield: bfloat16 [10240, 32, 1024], P('freq', 'rows'), may hold values from -6 to 6
- u_factors: bfloat16 [2, 16, 4, 256, 512], P(None, 'freq', 'rows'), may hold values from -0.25 to 0.25
- v_factors: bfloat16 [2, 16, 4, 512, 256], P(None, 'freq', 'rows'), may hold values from -0.375 to 0.375
- tile_ranks: int32 [16, 4, 40], P('freq', 'rows'), may hold values from 1 to 64, as said below
- tile_offsets: int32 [16, 4, 40], P('freq', 'rows'), may hold values from 0 to 511, as said below
Outputs:
- convolved: bfloat16 [1024, 32, 1024], P(('rows', 'freq'))
The draws below stay inside these ranges and needn't reach their ends.
Inputs may be any that keep to these rules, and one draw needn't show every extreme that they name: tile_ranks[k, i, j] is the rank of tile (i, j) of frequency k; the ranks of one tile row sum to at most 512, exactly 512 on some row of every draw, and every tile row has a tile of rank 64. tile_offsets[k, i, j] is the sum of tile_ranks[k, i, j2] over j2 < j.
All inputs are finite; a program needn't handle non-finite values.
Results may differ from the reference program's by a relative error of at most 0.0072.
Values may be sent and summed in bfloat16 or wider, within the bound.
A program may use at most 128 MiB of HBM per device.

```python
import math
import jax
import jax.numpy as jnp
from jax import lax

RECEIVERS = 10240
SAMPLES = 1024
TILE = 256
RANK_MAX = 64
SLOTS = 512
SOURCES = 32
FREQS = 16
TILE_ROWS = 4
TILE_COLS = 40


def rank_tables(key):
    base_key = jax.random.fold_in(key, 4242)
    key_weight, key_target, key_chosen, key_peak = jax.random.split(base_key, 4)
    weight = jax.random.randint(key_weight, (FREQS, TILE_ROWS, TILE_COLS), 1, 65)
    weight = weight * weight // 64 + 1
    target = SLOTS // 2 + jax.random.randint(key_target, (FREQS, TILE_ROWS), 0, SLOTS - SLOTS // 2 + 1)
    chosen = jax.random.randint(key_chosen, (), 0, FREQS * TILE_ROWS)
    row_number = jnp.arange(FREQS * TILE_ROWS, dtype=jnp.int32).reshape(FREQS, TILE_ROWS)
    target = jnp.where(row_number == chosen, SLOTS, target)
    peak_tile = jax.random.randint(key_peak, (FREQS, TILE_ROWS, 1), 0, TILE_COLS)
    is_peak = jnp.arange(TILE_COLS, dtype=jnp.int32)[None, None, :] == peak_tile
    spare_slots = target - (TILE_COLS - 1) - RANK_MAX
    others = jnp.where(is_peak, 0, weight)
    weight_sum = jnp.sum(others, axis=2)
    base_rank = jnp.minimum(1 + others * spare_slots[:, :, None] // weight_sum[:, :, None], RANK_MAX)
    rank_table = jnp.where(is_peak, RANK_MAX, base_rank)
    deficit = target - jnp.sum(rank_table, axis=2)
    headroom = jnp.where(is_peak, 0, RANK_MAX - rank_table)
    before = jnp.cumsum(headroom, axis=2) - headroom
    rank_table = rank_table + jnp.clip(deficit[:, :, None] - before, 0, headroom)
    starts = jnp.cumsum(rank_table, axis=2) - rank_table
    return (rank_table.astype(jnp.int32), starts.astype(jnp.int32))


def draw_tile_ranks(key, part):
    return rank_tables(key)[0]


def draw_tile_offsets(key, part):
    return rank_tables(key)[1]


def level_of(rng, shape, cuts, least, top_value):
    def one(dim, parts):
        steps = jax.random.uniform(jax.random.fold_in(jax.random.fold_in(rng, 6), dim), (parts,), jnp.float32, least / len(cuts), top_value / len(cuts))
        return jnp.repeat(jnp.exp(steps), shape[dim] // parts).reshape((-1,) + (1,) * (len(shape) - dim - 1))

    gain = one(*cuts[0])
    for cut in cuts[1:]:
        gain = gain * one(*cut)
    return gain


def gaussian(stream_key, shape, spread, most, shards=(), kind=jnp.bfloat16):
    entries = jax.random.normal(stream_key, shape, jnp.float32) * spread
    if len(shards) > 0:
        entries = level_of(stream_key, shape, shards, -0.22, 0.18) * entries
    return jnp.clip(entries, min=-most, max=most).astype(kind)


def setup_inputs(seed: int = 0) -> dict:
    seeds = jax.random.split(jax.random.key(seed), 6)
    return {
        "wavefield": gaussian(seeds[0], (RECEIVERS, SOURCES, SAMPLES), 1.0, 6.0, ((0, 8), (1, 4))),
        "u_factors": gaussian(seeds[1], (2, FREQS, TILE_ROWS, TILE, SLOTS), SLOTS ** -0.5, 0.25, ((1, 8), (2, 4))),
        "v_factors": gaussian(seeds[2], (2, FREQS, TILE_ROWS, SLOTS, TILE), TILE ** -0.5, 0.375, ((1, 8), (2, 4))),
        "tile_ranks": draw_tile_ranks(jax.random.fold_in(seeds[5], 71), 0),
        "tile_offsets": draw_tile_offsets(jax.random.fold_in(seeds[5], 71), 0),
    }


def spectral_tables(freq_count, sample_count):
    freq_bins = jnp.arange(freq_count, dtype=jnp.int32) + 1
    sample_index = jnp.arange(sample_count, dtype=jnp.int32)
    phase_int = freq_bins[:, None] * sample_index[None, :] % sample_count
    angles = phase_int.astype(jnp.float32) * (2.0 * math.pi / sample_count)
    cosine = jnp.cos(angles)
    minus_sine = -jnp.sin(angles)
    stacked = jnp.stack([cosine, minus_sine], axis=1)
    forward = (stacked / math.sqrt(sample_count)).astype(jnp.bfloat16)
    inverse = (stacked / math.sqrt(freq_count)).astype(jnp.bfloat16)
    return (forward, inverse)

def tile_windows(v_row, u_row, starts, rank_max):
    columns = starts.shape[0]
    slot_index = (starts[:, None] + jnp.arange(rank_max, dtype=jnp.int32)[None, :]).reshape(-1)
    v_padded = jnp.pad(v_row, ((0, 0), (0, rank_max), (0, 0)))
    u_padded = jnp.pad(u_row, ((0, 0), (0, 0), (0, rank_max)))
    v_win = jnp.take(v_padded, slot_index, axis=1).reshape(2, columns, rank_max, v_row.shape[2])
    u_win = jnp.take(u_padded, slot_index, axis=2).reshape(2, u_row.shape[1], columns, rank_max)
    return (v_win, u_win)

def tile_row_product(u_row, v_row, counts, starts, spectra):
    v_win, u_win = tile_windows(v_row, u_row, starts, RANK_MAX)
    quadrants = jnp.einsum('ajmr,jbrs->abjms', v_win.astype(jnp.float32), spectra.astype(jnp.float32))
    real_part = quadrants[0, 0] - quadrants[1, 1]
    imag_part = quadrants[0, 1] + quadrants[1, 0]
    rank_mask = jnp.arange(RANK_MAX, dtype=jnp.int32)[None, :] < counts[:, None]
    coeffs = jnp.where(rank_mask[None, :, :, None], jnp.stack([real_part, imag_part]), 0.0).astype(jnp.bfloat16)
    products = jnp.einsum('arjm,cjms->acrs', u_win.astype(jnp.float32), coeffs.astype(jnp.float32))
    return jnp.stack([products[0, 0] - products[1, 1], products[0, 1] + products[1, 0]]).astype(jnp.bfloat16)

def reference(wavefield, u_factors, v_factors, tile_ranks, tile_offsets):
    receivers, sources, samples = wavefield.shape
    freqs = u_factors.shape[1]
    tile_rows = u_factors.shape[2]
    tile_size = u_factors.shape[3]
    columns = receivers // tile_size
    forward, inverse = spectral_tables(freqs, samples)
    blocks = wavefield.reshape(columns, tile_size, sources, samples)

    def transform(block):
        return jnp.einsum('kct,rst->kcrs', forward.astype(jnp.float32), block.astype(jnp.float32)).astype(jnp.bfloat16)
    spectrum = jnp.moveaxis(lax.map(transform, blocks), 1, 0)

    def one_band(items):
        spectra, u_band, v_band, counts, starts = items
        rows_out = [tile_row_product(u_band[:, tile_row], v_band[:, tile_row], counts[tile_row], starts[tile_row], spectra) for tile_row in range(tile_rows)]
        return jnp.stack(rows_out, axis=1)
    bands = lax.map(one_band, (spectrum, jnp.moveaxis(u_factors, 1, 0), jnp.moveaxis(v_factors, 1, 0), tile_ranks, tile_offsets))
    flat_bands = bands.reshape(freqs, 2, tile_rows * tile_size * sources)
    series = jnp.einsum('kcq,kct->qt', flat_bands.astype(jnp.float32), inverse.astype(jnp.float32))
    return series.reshape(tile_rows * tile_size, sources, samples).astype(jnp.bfloat16)
```

```python
import functools
import math

import jax
import jax.numpy as jnp
import numpy as np
from jax import lax
from jax.experimental import pallas as pl
from jax.experimental.pallas import tpu as pltpu
from jax.sharding import PartitionSpec as P

RANK_MAX = 64
MESH = pl.DeviceIdType.MESH
LANES = 128
LAG = 3


def spectral_tables(freq_count, sample_count):
    freq_bins = jnp.arange(freq_count, dtype=jnp.int32) + 1
    sample_index = jnp.arange(sample_count, dtype=jnp.int32)
    phase_int = freq_bins[:, None] * sample_index[None, :] % sample_count
    angles = phase_int.astype(jnp.float32) * (2.0 * math.pi / sample_count)
    cosine = jnp.cos(angles)
    minus_sine = -jnp.sin(angles)
    stacked = jnp.stack([cosine, minus_sine], axis=1)
    forward = (stacked / math.sqrt(sample_count)).astype(jnp.bfloat16)
    inverse = (stacked / math.sqrt(freq_count)).astype(jnp.bfloat16)
    return (forward, inverse)


def tile_windows(v_row, u_row, starts, rank_max):
    columns = starts.shape[0]
    slot_index = (starts[:, None] + jnp.arange(rank_max, dtype=jnp.int32)[None, :]).reshape(-1)
    v_padded = jnp.pad(v_row, ((0, 0), (0, rank_max), (0, 0)))
    u_padded = jnp.pad(u_row, ((0, 0), (0, 0), (0, rank_max)))
    v_win = jnp.take(v_padded, slot_index, axis=1).reshape(2, columns, rank_max, v_row.shape[2])
    u_win = jnp.take(u_padded, slot_index, axis=2).reshape(2, u_row.shape[1], columns, rank_max)
    return (v_win, u_win)


def slot_lookup(starts, counts, rank_max, slot_count):
    position = jnp.arange(slot_count, dtype=jnp.int32)
    started = starts[:, None, :] <= position[None, :, None]
    owner_tile = jnp.sum(started.astype(jnp.int32), axis=2) - 1
    first_slot = jnp.max(jnp.where(started, starts[:, None, :], 0), axis=2)
    within = position[None, :] - first_slot
    live_slot = position[None, :] < (starts[:, -1] + counts[:, -1])[:, None]
    flat_index = jnp.where(live_slot, owner_tile * rank_max + within, 0)
    return (flat_index, live_slot)


def take_slots(values, chosen):
    return jnp.take(values, chosen, axis=1)


def general_device(wavefield, u_factors, v_factors, tile_ranks, tile_offsets):
    rec_dev, src_dev, samples = wavefield.shape
    freq_dev = u_factors.shape[1]
    rows_dev = u_factors.shape[2]
    tile_size = u_factors.shape[3]
    slot_count = u_factors.shape[4]
    freq_group = lax.axis_size("freq")
    row_group = lax.axis_size("rows")
    freqs = freq_dev * freq_group
    receivers = rec_dev * freq_group
    columns = receivers // tile_size
    sources = src_dev * row_group
    forward, inverse = spectral_tables(freqs, samples)
    spectrum = jnp.einsum("kct,rst->kcrs", forward, wavefield, preferred_element_type=jnp.float32)
    spectrum = spectrum.astype(jnp.bfloat16).reshape(freqs, 2, rec_dev * src_dev)
    windows = jax.vmap(
        functools.partial(tile_windows, rank_max=RANK_MAX), in_axes=(1, 1, 0), out_axes=(1, 1)
    )
    rank_slots = jnp.arange(RANK_MAX, dtype=jnp.int32)
    tile_row = 0
    v_win, u_win = windows(
        v_factors[:, :, tile_row], u_factors[:, :, tile_row], tile_offsets[:, tile_row]
    )
    rank_mask = rank_slots[None, None, :] < tile_ranks[:, tile_row, :, None]
    flat_index, live_slot = slot_lookup(
        tile_offsets[:, tile_row], tile_ranks[:, tile_row], RANK_MAX, slot_count
    )
    prepared = [(v_win, u_win, rank_mask, flat_index, live_slot)]
    by_frequency = lax.all_to_all(spectrum, "freq", split_axis=0, concat_axis=2, tiled=True)
    portion = lax.all_gather(by_frequency[None], "rows", axis=0, tiled=True)
    blocks_in = portion.shape[0]
    spectra = portion.reshape(blocks_in, freq_dev, 2, columns, tile_size, src_dev)
    spectra = jnp.transpose(spectra, (1, 2, 3, 4, 0, 5)).reshape(
        freq_dev, 2, columns, tile_size, blocks_in * src_dev
    )
    tile_row = 0
    v_win, u_win, rank_mask, flat_index, live_slot = prepared[tile_row]
    quadrants = jnp.einsum(
        "afjmr,fbjrs->fabjms", v_win, spectra, preferred_element_type=jnp.float32
    )
    coeffs = jnp.stack(
        [quadrants[:, 0, 0] - quadrants[:, 1, 1], quadrants[:, 0, 1] + quadrants[:, 1, 0]], axis=1
    )
    coeffs = jnp.where(rank_mask[:, None, :, :, None], coeffs, 0.0).astype(jnp.bfloat16)
    stacked = coeffs.reshape(freq_dev, 2, columns * RANK_MAX, blocks_in * src_dev)
    packed = jax.vmap(take_slots)(stacked, flat_index)
    packed = jnp.where(live_slot[:, None, :, None], packed, jnp.zeros((), jnp.bfloat16))
    products = jnp.einsum(
        "afrk,fcks->facrs", u_factors[:, :, tile_row], packed, preferred_element_type=jnp.float32
    )
    results = [
        jnp.stack(
            [products[:, 0, 0] - products[:, 1, 1], products[:, 0, 1] + products[:, 1, 0]], axis=1
        )
    ]
    merged = jnp.stack(results, axis=2)
    bands = merged.astype(jnp.bfloat16).reshape(
        freq_dev, 2, rows_dev * tile_size, blocks_in, src_dev
    )
    bands = bands.reshape(freq_dev, 2, rows_dev * tile_size * sources)
    returned = lax.all_to_all(bands, "freq", split_axis=2, concat_axis=0, tiled=True)
    series = jnp.einsum("kcq,kct->qt", returned, inverse, preferred_element_type=jnp.float32)
    return series.astype(jnp.bfloat16).reshape(rows_dev * tile_size // freq_group, sources, samples)


def host_tables(freq_count, sample_count):
    freq_bins = np.arange(freq_count) + 1
    phase = freq_bins[:, None] * np.arange(sample_count)[None, :] % sample_count
    angles = phase * (2.0 * math.pi / sample_count)
    stacked = np.stack([np.cos(angles), -np.sin(angles)], axis=1)
    stacked = stacked.reshape(2 * freq_count, sample_count)
    forward = (stacked / math.sqrt(sample_count)).astype(np.float32)
    inverse = (stacked / math.sqrt(freq_count)).astype(np.float32)
    return forward, inverse


def band_kernel(
    groups, chunks, tile, src_dev,
    wave, table_hbm, u_hbm, v_hbm, starts_hbm, counts_hbm, out_ref,
    starts, counts, table, u_ref, v_ref, owner, wbuf, spec, send, xbuf, acc, bsend, brecv,
    isem, tsem, usem, vsem, wsem, sa, ra, sx, rx, sf, rv, ru, ro, sb, rb,
):
    me = lax.axis_index("freq")
    row = lax.axis_index("rows")
    core = lax.rem(row, 2)
    side = row // 2
    across = lax.rem(row + 2, 4)
    partner = row + 1 - 2 * core
    half = groups // 2
    own_half = me // half
    steps = 2 * chunks
    width = tile // 2
    freq_dev = owner.shape[1]
    slots = owner.shape[3]
    piece = send.shape[1] // groups
    factors = u_ref.shape[1]
    step_rows = width * src_dev

    def load(h):
        return pltpu.make_async_copy(
            wave.at[pl.ds(h * step_rows, step_rows)], wbuf.at[h], wsem.at[h]
        )

    load_table = pltpu.make_async_copy(table_hbm, table, tsem)
    load_v = pltpu.make_async_copy(v_hbm, v_ref.at[0], vsem)
    load_u = pltpu.make_async_copy(u_hbm, u_ref.at[0], usem)
    load_starts = pltpu.make_async_copy(starts_hbm, starts, isem.at[0])
    load_counts = pltpu.make_async_copy(counts_hbm, counts, isem.at[1])
    load(0).start()
    load_table.start()
    load_starts.start()
    load_counts.start()

    barrier = pltpu.get_barrier_semaphore()

    def greet(d, carry):
        peer = lax.rem(me + d, groups)
        pl.semaphore_signal(barrier, inc=1, device_id=(peer, row), device_id_type=MESH)
        pl.semaphore_signal(barrier, inc=1, device_id=(peer, partner), device_id_type=MESH)
        return carry

    lax.fori_loop(1, groups, greet, 0)
    pl.semaphore_signal(barrier, inc=1, device_id=(me, across), device_id_type=MESH)
    pl.semaphore_signal(barrier, inc=1, device_id=(me, partner), device_id_type=MESH)

    def start_load(h, carry):
        load(h).start()
        return carry

    lax.fori_loop(1, steps, start_load, 0)
    load_v.start()
    load_u.start()

    load_starts.wait()
    load_counts.wait()
    slot = lax.broadcasted_iota(jnp.int32, (8, slots), 1)
    for k in range(freq_dev):
        tiles = groups * chunks

        def count_started(j, held):
            return held + (slot >= starts[k, j]).astype(jnp.int32)

        held = lax.fori_loop(0, tiles, count_started, jnp.full((8, slots), -1, jnp.int32), unroll=8)
        live = slot < starts[k, tiles - 1] + counts[k, tiles - 1]
        owner[0, k] = jnp.where(live, held, -1)
    acc[...] = jnp.zeros_like(acc)
    lane_mod = lax.rem(lax.broadcasted_iota(jnp.int32, (width, LANES), 1), src_dev)

    def exchange(h, peer, sender, r_sem):
        return pltpu.make_async_remote_copy(
            src_ref=send.at[h, pl.ds(peer * piece, piece)],
            dst_ref=xbuf.at[h, side, sender],
            send_sem=sa,
            recv_sem=r_sem,
            device_id=(peer, row),
            device_id_type=MESH,
        )

    def cross(h, first, count, block):
        return pltpu.make_async_remote_copy(
            src_ref=xbuf.at[h, block, pl.ds(first, count)],
            dst_ref=xbuf.at[h, block, pl.ds(first, count)],
            send_sem=sx,
            recv_sem=rx.at[h],
            device_id=(me, across),
            device_id_type=MESH,
        )

    def to_partner(src, dst, r_sem):
        return pltpu.make_async_remote_copy(
            src_ref=src,
            dst_ref=dst,
            send_sem=sf,
            recv_sem=r_sem,
            device_id=(me, partner),
            device_id_type=MESH,
        )

    def share_v(n):
        return to_partner(v_hbm.at[n], v_ref.at[1, n], rv)

    def share_u(n):
        return to_partner(u_hbm.at[n], u_ref.at[1, n], ru)

    share_owner = to_partner(owner.at[0], owner.at[1], ro)

    def transform(h):
        load(h).wait()
        values = lax.dot_general(
            wbuf[h], table[...], (((1,), (0,)), ((), ())),
            preferred_element_type=jnp.float32,
        )
        for p in range(spec.shape[0]):
            spec[p] = values[:, p * LANES : (p + 1) * LANES]
        for p in range(spec.shape[0]):
            cols = slice(p * LANES, (p + 1) * LANES)
            picked = spec[p, pl.ds(0, width, stride=src_dev), :]
            for s in range(1, src_dev):
                picked = jnp.where(
                    lane_mod == s, spec[p, pl.ds(s, width, stride=src_dev), :], picked
                )
            send[h, cols, :] = picked.T.astype(jnp.bfloat16)
        own = pl.multiple_of(me * piece, piece)
        xbuf[h, side, me] = send[h, pl.ds(own, piece), :]

    def distribute(h):
        cross(h, me, 1, side).start()
        for d in range(1, half):
            peer = own_half * half + lax.rem(me + d, half)
            exchange(h, peer, me, ra.at[h, 0]).start()
        for d in range(half):
            peer = (1 - own_half) * half + lax.rem(me + d, half)
            exchange(h, peer, me, ra.at[h, 1]).start()

    def relay_near(h):
        pltpu.make_async_copy(
            xbuf.at[h, side, pl.ds(0, half - 1)], xbuf.at[h, side, pl.ds(0, half - 1)], ra.at[h, 0]
        ).wait()
        for d in range(1, half):
            cross(h, own_half * half + lax.rem(me + d, half), 1, side).start()

    def relay_far(h):
        pltpu.make_async_copy(
            xbuf.at[h, side, pl.ds(0, half)], xbuf.at[h, side, pl.ds(0, half)], ra.at[h, 1]
        ).wait()
        cross(h, (1 - own_half) * half, half, side).start()

    def project(c):
        for n in range(2):
            cross(2 * c + n, 0, groups, 1 - side).wait_recv()
        rows = 2 * src_dev
        for k in range(freq_dev):
            parts = [
                xbuf[2 * c + n, :, :, k * rows : (k + 1) * rows, :].reshape(2 * groups * rows, width)
                for n in range(2)
            ]
            left = jnp.concatenate(parts, axis=1)
            for i in range(2):
                held = owner[i, k]
                inside = [(held == g * chunks + c)[0:1] for g in range(groups)]
                for a in range(2):
                    products = lax.dot_general(
                        left, v_ref[i, a * freq_dev + k], (((1,), (1,)), ((), ())),
                        preferred_element_type=jnp.float32,
                    ).reshape(2, groups, rows, slots)
                    total = acc[i, k, a]
                    for g in range(groups):
                        total = jnp.where(inside[g][None], products[:, g], total)
                    acc[i, k, a] = total

    def first_pass(h, carry):
        transform(h)
        pl.when(h == 0)(lambda: pl.semaphore_wait(barrier, 2 * groups))
        distribute(h)
        pl.when(h == 1)(share_owner.start)
        pl.when((h >= 2) & (h < 2 + factors))(lambda: share_v(h - 2).start())
        pl.when((h >= 2 + factors) & (h < 2 + 2 * factors))(lambda: share_u(h - 2 - factors).start())
        pl.when(h >= LAG)(lambda: relay_near(h - LAG))
        pl.when(h == LAG + 2)(lambda: relay_far(0))
        pl.when(h > 2 * LAG)(lambda: relay_far(h - 2 * LAG))
        return carry

    load_table.wait()
    lax.fori_loop(0, steps, first_pass, 0)
    load_v.wait()
    to_partner(v_ref.at[0], v_ref.at[1], rv).wait_recv()
    share_owner.wait_recv()

    near_turn = {steps - LAG + n: n for n in range(LAG)}
    far_turn = {}
    for c in range(chunks):
        for h in range(steps - 2 * LAG, min(steps, max(2 * c + 4, steps + 1 - 2 * LAG + c))):
            far_turn.setdefault(h, c)

    def second_pass(c, carry):
        for h, turn in far_turn.items():
            pl.when(c == turn)(functools.partial(relay_far, h))
        for h, turn in near_turn.items():
            pl.when(c == turn)(functools.partial(relay_near, h))
        project(c)
        return carry

    lax.fori_loop(0, chunks, second_pass, 0)

    load_u.wait()
    to_partner(u_ref.at[0], u_ref.at[1], ru).wait_recv()

    def give_back(i, peer):
        return pltpu.make_async_remote_copy(
            src_ref=bsend.at[i, peer],
            dst_ref=brecv.at[core * groups + me],
            send_sem=sb,
            recv_sem=rb,
            device_id=(peer, partner if i else row),
            device_id_type=MESH,
        )

    contract = (((1,), (1,)), ((), ()))
    sources = 2 * src_dev
    q_low = LANES // (2 * sources)
    q_high = tile // groups // q_low
    for i in (1, 0):
        rows_out = []
        for k in range(freq_dev):
            first = acc[i, k, 0].reshape(2, 2, src_dev, slots)
            second = acc[i, k, 1].reshape(2, 2, src_dev, slots)
            real = (first[:, 0] - second[:, 1]).reshape(sources, slots)
            imag = (first[:, 1] + second[:, 0]).reshape(sources, slots)
            straight = jnp.concatenate([real, imag], axis=0).astype(jnp.bfloat16)
            turned = jnp.concatenate([-imag, real], axis=0).astype(jnp.bfloat16)
            band = lax.dot_general(
                u_ref[i, k], straight, contract, preferred_element_type=jnp.float32
            )
            band = band + lax.dot_general(
                u_ref[i, freq_dev + k], turned, contract, preferred_element_type=jnp.float32
            )
            split = band.reshape(groups, q_low, q_high, 2 * sources)
            rows_out.append(jnp.concatenate([split[:, q] for q in range(q_low)], axis=-1))
        bsend[i] = jnp.concatenate(rows_out, axis=1).astype(jnp.bfloat16)

    def start_back(d, carry):
        give_back(1, lax.rem(me + groups // 2 + d, groups)).start()
        pl.when(d != groups // 2)(lambda: give_back(0, lax.rem(me + groups // 2 + d, groups)).start())
        return carry

    lax.fori_loop(0, groups, start_back, 0)
    brecv[core * groups + me] = bsend[0, me]

    sent = send.at[:, pl.ds(0, (groups - 1) * piece)]
    pltpu.make_async_copy(sent, sent, sa).wait()
    pltpu.make_async_copy(xbuf.at[:, 0], xbuf.at[:, 0], sx).wait()
    pltpu.make_async_copy(v_ref.at[0], v_ref.at[0], sf).wait()
    pltpu.make_async_copy(u_ref.at[0], u_ref.at[0], sf).wait()
    pltpu.make_async_copy(owner.at[0], owner.at[0], sf).wait()
    arrived = brecv.at[pl.ds(0, 2 * groups - 1)]
    pltpu.make_async_copy(arrived, arrived, sb).wait()
    pltpu.make_async_copy(arrived, arrived, rb).wait()
    out_ref[...] = brecv[...].reshape(out_ref.shape)


def series_kernel(band_ref, table_ref, out_hbm, wide, out, sem):
    q_low, q_high, sources, samples = out.shape
    block = band_ref.shape[0] // 2
    half = sources // 2
    low = band_ref[:block, :].astype(jnp.float32)
    high = band_ref[block:, :].astype(jnp.float32)
    first = lax.broadcasted_iota(jnp.int32, low.shape, 1) % sources < half
    wide[0] = jnp.where(first, low, pltpu.roll(high, half, 1))
    wide[1] = jnp.where(first, pltpu.roll(low, LANES - half, 1), high)

    for q in range(q_high):
        rows = pl.ds(q, block // q_high, stride=q_high)
        left = jnp.concatenate([wide[0, rows, :], wide[1, rows, :]], axis=0).T
        left = left.reshape(q_low, 2, 2, half // 2, left.shape[1])
        left = jnp.swapaxes(left, 1, 2).reshape(q_low * sources, left.shape[-1])
        series = jnp.dot(
            left.astype(jnp.bfloat16), table_ref[...], preferred_element_type=jnp.float32
        )
        out[:, q] = series.astype(jnp.bfloat16).reshape(q_low, sources, samples)
        pltpu.make_async_copy(out.at[:, q], out_hbm.at[:, q], sem).start()
    pltpu.make_async_copy(out, out_hbm, sem).wait()


def fast_device(wavefield, u_factors, v_factors, tile_ranks, tile_offsets):
    rec_dev, src_dev, samples = wavefield.shape
    freq_dev, tile, slots = u_factors.shape[1], u_factors.shape[3], u_factors.shape[4]
    groups = lax.axis_size("freq")
    chunks = rec_dev // tile
    steps, width = 2 * chunks, tile // 2
    freqs = freq_dev * groups
    forward, inverse = host_tables(freqs, samples)
    table = jnp.asarray(np.repeat(forward.T, src_dev, axis=1)).astype(jnp.bfloat16)
    inverse = inverse.reshape(freqs, 2, samples).transpose(1, 0, 2).reshape(2 * freqs, samples)
    inverse = jnp.asarray(inverse).astype(jnp.bfloat16)
    columns = table.shape[1]
    piece = columns // groups
    sources = 4 * src_dev
    q_dev = tile // groups
    q_low = LANES // sources
    q_high = q_dev // q_low
    band_rows = freq_dev * q_high
    factors = 2 * freq_dev
    vmem = pl.BlockSpec(memory_space=pltpu.VMEM)
    hbm = pl.BlockSpec(memory_space=pl.ANY)
    dma = pltpu.SemaphoreType.DMA
    bands = pl.pallas_call(
        functools.partial(band_kernel, groups, chunks, tile, src_dev),
        out_shape=jax.ShapeDtypeStruct((2 * groups * band_rows, LANES), jnp.bfloat16),
        in_specs=[hbm] * 6,
        out_specs=vmem,
        scratch_shapes=[
            pltpu.SMEM(tile_offsets[:, 0].shape, jnp.int32),
            pltpu.SMEM(tile_ranks[:, 0].shape, jnp.int32),
            pltpu.VMEM((samples, columns), jnp.bfloat16),
            pltpu.VMEM((2, factors, tile, slots), jnp.bfloat16),
            pltpu.VMEM((2, factors, slots, tile), jnp.bfloat16),
            pltpu.VMEM((2, freq_dev, 8, slots), jnp.int32),
            pltpu.VMEM((steps, width * src_dev, samples), jnp.bfloat16),
            pltpu.VMEM((columns // LANES, width * src_dev, LANES), jnp.float32),
            pltpu.VMEM((steps, columns, width), jnp.bfloat16),
            pltpu.VMEM((steps, 2, groups, piece, width), jnp.bfloat16),
            pltpu.VMEM((2, freq_dev, 2, 2, 2 * src_dev, slots), jnp.float32),
            pltpu.VMEM((2, groups, band_rows, LANES), jnp.bfloat16),
            pltpu.VMEM((2 * groups, band_rows, LANES), jnp.bfloat16),
            dma((2,)), dma, dma, dma, dma((steps,)),
            dma, dma((steps, 2)), dma, dma((steps,)),
            dma, dma, dma, dma, dma, dma,
        ],
        compiler_params=pltpu.CompilerParams(
            collective_id=0, has_side_effects=True, vmem_limit_bytes=60 * 1024 * 1024
        ),
        name="bands",
    )(
        wavefield.reshape(rec_dev * src_dev, samples),
        table,
        u_factors.reshape(factors, tile, slots),
        v_factors.reshape(factors, slots, tile),
        tile_offsets[:, 0],
        tile_ranks[:, 0],
    )
    shape = (q_low, q_high, sources, samples)
    series = pl.pallas_call(
        series_kernel,
        out_shape=jax.ShapeDtypeStruct(shape, jnp.bfloat16),
        in_specs=[vmem, vmem],
        out_specs=hbm,
        scratch_shapes=[
            pltpu.VMEM((2, bands.shape[0] // 2, LANES), jnp.float32),
            pltpu.VMEM(shape, jnp.bfloat16),
            dma,
        ],
        name="series",
    )(bands, inverse)
    return series.reshape(q_dev, sources, samples)


def per_device(wavefield, u_factors, v_factors, tile_ranks, tile_offsets):
    rec_dev, src_dev, samples = wavefield.shape
    tile, slots = u_factors.shape[3], u_factors.shape[4]
    groups = lax.axis_size("freq")
    aligned = tile % LANES == 0 and rec_dev % tile == 0 and slots % LANES == 0
    aligned = aligned and samples % LANES == 0
    counts = u_factors.shape[1] == 2 and u_factors.shape[2] == 1 and src_dev == 8
    counts = counts and lax.axis_size("rows") == 4 and groups % 2 == 0
    if aligned and counts and tile == groups * 32:
        return fast_device(wavefield, u_factors, v_factors, tile_ranks, tile_offsets)
    return general_device(wavefield, u_factors, v_factors, tile_ranks, tile_offsets)


def solution(mesh):
    placed = (
        P("freq", "rows", None),
        P(None, "freq", "rows", None, None),
        P(None, "freq", "rows", None, None),
        P("freq", "rows", None),
        P("freq", "rows", None),
    )
    return jax.shard_map(
        per_device,
        mesh=mesh,
        in_specs=placed,
        out_specs=P(("rows", "freq"), None, None),
        check_vma=False,
    )
```

```python
import functools
import math

import jax
import jax.numpy as jnp
import numpy as np
from jax import lax
from jax.experimental import pallas as pl
from jax.experimental.pallas import tpu as pltpu
from jax.sharding import PartitionSpec as P

RANK_MAX = 64
MESH = pl.DeviceIdType.MESH
LANES = 128
LAG = 3


def spectral_tables(freq_count, sample_count):
    freq_bins = jnp.arange(freq_count, dtype=jnp.int32) + 1
    sample_index = jnp.arange(sample_count, dtype=jnp.int32)
    phase_int = freq_bins[:, None] * sample_index[None, :] % sample_count
    angles = phase_int.astype(jnp.float32) * (2.0 * math.pi / sample_count)
    cosine = jnp.cos(angles)
    minus_sine = -jnp.sin(angles)
    stacked = jnp.stack([cosine, minus_sine], axis=1)
    forward = (stacked / math.sqrt(sample_count)).astype(jnp.bfloat16)
    inverse = (stacked / math.sqrt(freq_count)).astype(jnp.bfloat16)
    return (forward, inverse)


def tile_windows(v_row, u_row, starts, rank_max):
    columns = starts.shape[0]
    slot_index = (starts[:, None] + jnp.arange(rank_max, dtype=jnp.int32)[None, :]).reshape(-1)
    v_padded = jnp.pad(v_row, ((0, 0), (0, rank_max), (0, 0)))
    u_padded = jnp.pad(u_row, ((0, 0), (0, 0), (0, rank_max)))
    v_win = jnp.take(v_padded, slot_index, axis=1).reshape(2, columns, rank_max, v_row.shape[2])
    u_win = jnp.take(u_padded, slot_index, axis=2).reshape(2, u_row.shape[1], columns, rank_max)
    return (v_win, u_win)


def slot_lookup(starts, counts, rank_max, slot_count):
    position = jnp.arange(slot_count, dtype=jnp.int32)
    started = starts[:, None, :] <= position[None, :, None]
    owner_tile = jnp.sum(started.astype(jnp.int32), axis=2) - 1
    first_slot = jnp.max(jnp.where(started, starts[:, None, :], 0), axis=2)
    within = position[None, :] - first_slot
    live_slot = position[None, :] < (starts[:, -1] + counts[:, -1])[:, None]
    flat_index = jnp.where(live_slot, owner_tile * rank_max + within, 0)
    return (flat_index, live_slot)


def take_slots(values, chosen):
    return jnp.take(values, chosen, axis=1)


def general_device(wavefield, u_factors, v_factors, tile_ranks, tile_offsets):
    rec_dev, src_dev, samples = wavefield.shape
    freq_dev = u_factors.shape[1]
    rows_dev = u_factors.shape[2]
    tile_size = u_factors.shape[3]
    slot_count = u_factors.shape[4]
    freq_group = lax.axis_size("freq")
    row_group = lax.axis_size("rows")
    freqs = freq_dev * freq_group
    receivers = rec_dev * freq_group
    columns = receivers // tile_size
    sources = src_dev * row_group
    forward, inverse = spectral_tables(freqs, samples)
    spectrum = jnp.einsum("kct,rst->kcrs", forward, wavefield, preferred_element_type=jnp.float32)
    spectrum = spectrum.astype(jnp.bfloat16).reshape(freqs, 2, rec_dev * src_dev)
    windows = jax.vmap(
        functools.partial(tile_windows, rank_max=RANK_MAX), in_axes=(1, 1, 0), out_axes=(1, 1)
    )
    rank_slots = jnp.arange(RANK_MAX, dtype=jnp.int32)
    tile_row = 0
    v_win, u_win = windows(
        v_factors[:, :, tile_row], u_factors[:, :, tile_row], tile_offsets[:, tile_row]
    )
    rank_mask = rank_slots[None, None, :] < tile_ranks[:, tile_row, :, None]
    flat_index, live_slot = slot_lookup(
        tile_offsets[:, tile_row], tile_ranks[:, tile_row], RANK_MAX, slot_count
    )
    prepared = [(v_win, u_win, rank_mask, flat_index, live_slot)]
    by_frequency = lax.all_to_all(spectrum, "freq", split_axis=0, concat_axis=2, tiled=True)
    portion = lax.all_gather(by_frequency[None], "rows", axis=0, tiled=True)
    blocks_in = portion.shape[0]
    spectra = portion.reshape(blocks_in, freq_dev, 2, columns, tile_size, src_dev)
    spectra = jnp.transpose(spectra, (1, 2, 3, 4, 0, 5)).reshape(
        freq_dev, 2, columns, tile_size, blocks_in * src_dev
    )
    tile_row = 0
    v_win, u_win, rank_mask, flat_index, live_slot = prepared[tile_row]
    quadrants = jnp.einsum(
        "afjmr,fbjrs->fabjms", v_win, spectra, preferred_element_type=jnp.float32
    )
    coeffs = jnp.stack(
        [quadrants[:, 0, 0] - quadrants[:, 1, 1], quadrants[:, 0, 1] + quadrants[:, 1, 0]], axis=1
    )
    coeffs = jnp.where(rank_mask[:, None, :, :, None], coeffs, 0.0).astype(jnp.bfloat16)
    stacked = coeffs.reshape(freq_dev, 2, columns * RANK_MAX, blocks_in * src_dev)
    packed = jax.vmap(take_slots)(stacked, flat_index)
    packed = jnp.where(live_slot[:, None, :, None], packed, jnp.zeros((), jnp.bfloat16))
    products = jnp.einsum(
        "afrk,fcks->facrs", u_factors[:, :, tile_row], packed, preferred_element_type=jnp.float32
    )
    results = [
        jnp.stack(
            [products[:, 0, 0] - products[:, 1, 1], products[:, 0, 1] + products[:, 1, 0]], axis=1
        )
    ]
    merged = jnp.stack(results, axis=2)
    bands = merged.astype(jnp.bfloat16).reshape(
        freq_dev, 2, rows_dev * tile_size, blocks_in, src_dev
    )
    bands = bands.reshape(freq_dev, 2, rows_dev * tile_size * sources)
    returned = lax.all_to_all(bands, "freq", split_axis=2, concat_axis=0, tiled=True)
    series = jnp.einsum("kcq,kct->qt", returned, inverse, preferred_element_type=jnp.float32)
    return series.astype(jnp.bfloat16).reshape(rows_dev * tile_size // freq_group, sources, samples)


def host_tables(freq_count, sample_count):
    freq_bins = np.arange(freq_count) + 1
    phase = freq_bins[:, None] * np.arange(sample_count)[None, :] % sample_count
    angles = phase * (2.0 * math.pi / sample_count)
    stacked = np.stack([np.cos(angles), -np.sin(angles)], axis=1)
    stacked = stacked.reshape(2 * freq_count, sample_count)
    forward = (stacked / math.sqrt(sample_count)).astype(np.float32)
    inverse = (stacked / math.sqrt(freq_count)).astype(np.float32)
    return forward, inverse


def band_kernel(
    groups, chunks, tile, src_dev,
    wave, table_hbm, u_hbm, v_hbm, starts_hbm, counts_hbm, out_hbm,
    starts, counts, table, u_ref, v_ref, owner, wbuf, spec, send, xbuf, acc, bsend,
    isem, tsem, usem, vsem, wsem, sa, ra, sx, rx, sf, rv, ru, ro, sb, rb,
):
    me = lax.axis_index("freq")
    row = lax.axis_index("rows")
    core = lax.rem(row, 2)
    side = row // 2
    across = lax.rem(row + 2, 4)
    partner = row + 1 - 2 * core
    half = groups // 2
    quarter = groups // 4
    own_half = me // half
    place = me // quarter
    edge = 1 + (place * place - 3 * place) // 2
    steps = 2 * chunks
    width = tile // 2
    freq_dev = owner.shape[1]
    slots = owner.shape[3]
    piece = send.shape[1] // groups
    factors = u_ref.shape[1]
    step_rows = width * src_dev

    def load(h):
        return pltpu.make_async_copy(
            wave.at[pl.ds(h * step_rows, step_rows)], wbuf.at[h], wsem.at[h]
        )

    load_table = pltpu.make_async_copy(table_hbm, table, tsem)
    load_v = pltpu.make_async_copy(v_hbm, v_ref.at[0], vsem)
    load_u = pltpu.make_async_copy(u_hbm, u_ref.at[0], usem)
    load_starts = pltpu.make_async_copy(starts_hbm, starts, isem.at[0])
    load_counts = pltpu.make_async_copy(counts_hbm, counts, isem.at[1])
    load(0).start()
    load_table.start()
    load_starts.start()
    load_counts.start()

    barrier = pltpu.get_barrier_semaphore()

    def greet(d, carry):
        peer = lax.rem(me + d, groups)
        pl.semaphore_signal(barrier, inc=1, device_id=(peer, row), device_id_type=MESH)
        pl.semaphore_signal(barrier, inc=1, device_id=(peer, partner), device_id_type=MESH)
        return carry

    lax.fori_loop(1, groups, greet, 0)
    pl.semaphore_signal(barrier, inc=1, device_id=(me, across), device_id_type=MESH)
    pl.semaphore_signal(barrier, inc=1, device_id=(me, partner), device_id_type=MESH)

    def start_load(h, carry):
        load(h).start()
        return carry

    lax.fori_loop(1, steps, start_load, 0)
    load_v.start()
    load_u.start()

    load_starts.wait()
    load_counts.wait()
    slot = lax.broadcasted_iota(jnp.int32, (8, slots), 1)
    for k in range(freq_dev):
        tiles = groups * chunks

        def count_started(j, held):
            return held + (slot >= starts[k, j]).astype(jnp.int32)

        held = lax.fori_loop(0, tiles, count_started, jnp.full((8, slots), -1, jnp.int32), unroll=8)
        live = slot < starts[k, tiles - 1] + counts[k, tiles - 1]
        owner[0, k] = jnp.where(live, held, -1)
    acc[...] = jnp.zeros_like(acc)
    lane_mod = lax.rem(lax.broadcasted_iota(jnp.int32, (width, LANES), 1), src_dev)

    def exchange(h, peer, sender, r_sem):
        return pltpu.make_async_remote_copy(
            src_ref=send.at[h, pl.ds(peer * piece, piece)],
            dst_ref=xbuf.at[h, side, sender],
            send_sem=sa,
            recv_sem=r_sem,
            device_id=(peer, row),
            device_id_type=MESH,
        )

    def cross(h, first, count, block):
        return pltpu.make_async_remote_copy(
            src_ref=xbuf.at[h, block, pl.ds(first, count)],
            dst_ref=xbuf.at[h, block, pl.ds(first, count)],
            send_sem=sx,
            recv_sem=rx.at[h],
            device_id=(me, across),
            device_id_type=MESH,
        )

    def to_partner(src, dst, r_sem):
        return pltpu.make_async_remote_copy(
            src_ref=src,
            dst_ref=dst,
            send_sem=sf,
            recv_sem=r_sem,
            device_id=(me, partner),
            device_id_type=MESH,
        )

    def share_v(n):
        return to_partner(v_hbm.at[n], v_ref.at[1, n], rv)

    def share_u(n):
        return to_partner(u_hbm.at[n], u_ref.at[1, n], ru)

    share_owner = to_partner(owner.at[0], owner.at[1], ro)

    def transform(h):
        load(h).wait()
        values = lax.dot_general(
            wbuf[h], table[...], (((1,), (0,)), ((), ())),
            preferred_element_type=jnp.float32,
        )
        for p in range(spec.shape[0]):
            spec[p] = values[:, p * LANES : (p + 1) * LANES]
        for p in range(spec.shape[0]):
            cols = slice(p * LANES, (p + 1) * LANES)
            picked = spec[p, pl.ds(0, width, stride=src_dev), :]
            for s in range(1, src_dev):
                picked = jnp.where(
                    lane_mod == s, spec[p, pl.ds(s, width, stride=src_dev), :], picked
                )
            send[h, cols, :] = picked.T.astype(jnp.bfloat16)
        own = pl.multiple_of(me * piece, piece)
        xbuf[h, side, me] = send[h, pl.ds(own, piece), :]

    def distribute(h):
        cross(h, me, 1, side).start()
        for d in range(1, half):
            peer = own_half * half + lax.rem(me + d, half)
            exchange(h, peer, me, ra.at[h, 0]).start()
        for d in range(half):
            peer = (1 - own_half) * half + lax.rem(me + d, half)
            exchange(h, peer, me, ra.at[h, 1 + edge]).start()

    def relay_near(h):
        pltpu.make_async_copy(
            xbuf.at[h, side, pl.ds(0, half - 1)], xbuf.at[h, side, pl.ds(0, half - 1)], ra.at[h, 0]
        ).wait()
        for d in range(1, half):
            cross(h, own_half * half + lax.rem(me + d, half), 1, side).start()

    def relay_far(h, outer):
        first = (1 - own_half) * 3 * quarter if outer else (2 - own_half) * quarter
        block = xbuf.at[h, side, pl.ds(first, quarter)]
        pltpu.make_async_copy(block, block, ra.at[h, 1 + outer]).wait()
        cross(h, first, quarter, side).start()

    def relay_inner(h):
        relay_far(h, 0)

    def relay_outer(h):
        relay_far(h, 1)

    def project(c):
        for n in range(2):
            cross(2 * c + n, 0, groups, 1 - side).wait_recv()
        rows = 2 * src_dev
        for k in range(freq_dev):
            parts = [
                xbuf[2 * c + n, :, :, k * rows : (k + 1) * rows, :].reshape(2 * groups * rows, width)
                for n in range(2)
            ]
            left = jnp.concatenate(parts, axis=1)
            for i in range(2):
                held = owner[i, k]
                inside = [(held == g * chunks + c)[0:1] for g in range(groups)]
                for a in range(2):
                    products = lax.dot_general(
                        left, v_ref[i, a * freq_dev + k], (((1,), (1,)), ((), ())),
                        preferred_element_type=jnp.float32,
                    ).reshape(2, groups, rows, slots)
                    total = acc[i, k, a]
                    for g in range(groups):
                        total = jnp.where(inside[g][None], products[:, g], total)
                    acc[i, k, a] = total

    def first_pass(h, carry):
        transform(h)
        pl.when(h == 0)(lambda: pl.semaphore_wait(barrier, 2 * groups))
        distribute(h)
        pl.when(h == 1)(share_owner.start)
        pl.when((h >= 2) & (h < 2 + factors))(lambda: share_v(h - 2).start())
        pl.when((h >= 2 + factors) & (h < 2 + 2 * factors))(lambda: share_u(h - 2 - factors).start())
        pl.when(h >= LAG)(lambda: relay_near(h - LAG))
        pl.when(h > LAG)(lambda: relay_outer(h - LAG - 1))
        pl.when((h > LAG + 1) & (lax.rem(h, 2) == 1))(lambda: relay_inner((h - LAG - 2) // 2))
        return carry

    load_table.wait()
    lax.fori_loop(0, steps, first_pass, 0)
    load_v.wait()
    to_partner(v_ref.at[0], v_ref.at[1], rv).wait_recv()
    share_owner.wait_recv()

    early = (steps - LAG - 1) // 2
    order = [("inner", early), ("near", steps - 3), ("outer", steps - 4)]
    order += [("near", steps - 2), ("project", 0), ("outer", steps - 3)]
    order += [("inner", early + 1), ("near", steps - 1), ("outer", steps - 2)]
    order += [("inner", early + 2), ("outer", steps - 1), ("inner", early + 3), ("project", 1)]
    order += [("inner", h) for h in range(early + 4, steps)]
    order += [("project", c) for c in range(2, chunks)]
    turns, turn = [], []
    for kind, n in order:
        if kind == "project":
            turns.append(turn)
            turn = []
        else:
            turn.append((kind, n))
    relays = {"near": relay_near, "inner": relay_inner, "outer": relay_outer}

    def second_pass(c, carry):
        for n, turn in enumerate(turns):
            if turn:
                pl.when(c == n)(lambda turn=turn: [relays[kind](h) for kind, h in turn] and None)
        project(c)
        return carry

    lax.fori_loop(0, chunks, second_pass, 0)

    load_u.wait()
    to_partner(u_ref.at[0], u_ref.at[1], ru).wait_recv()

    def give_back(i, peer):
        return pltpu.make_async_remote_copy(
            src_ref=bsend.at[i, peer],
            dst_ref=out_hbm.at[core * groups + me],
            send_sem=sb,
            recv_sem=rb,
            device_id=(peer, partner if i else row),
            device_id_type=MESH,
        )

    contract = (((1,), (1,)), ((), ()))
    sources = 2 * src_dev
    q_low = LANES // (2 * sources)
    q_high = tile // groups // q_low
    for i in (1, 0):
        rows_out = []
        for k in range(freq_dev):
            first = acc[i, k, 0].reshape(2, 2, src_dev, slots)
            second = acc[i, k, 1].reshape(2, 2, src_dev, slots)
            real = (first[:, 0] - second[:, 1]).reshape(sources, slots)
            imag = (first[:, 1] + second[:, 0]).reshape(sources, slots)
            straight = jnp.concatenate([real, imag], axis=0).astype(jnp.bfloat16)
            turned = jnp.concatenate([-imag, real], axis=0).astype(jnp.bfloat16)
            band = lax.dot_general(
                u_ref[i, k], straight, contract, preferred_element_type=jnp.float32
            )
            band = band + lax.dot_general(
                u_ref[i, freq_dev + k], turned, contract, preferred_element_type=jnp.float32
            )
            split = band.reshape(groups, q_low, q_high, 2 * sources)
            rows_out.append(jnp.concatenate([split[:, q] for q in range(q_low)], axis=-1))
        bsend[i] = jnp.concatenate(rows_out, axis=1).astype(jnp.bfloat16)

    def start_back(d, carry):
        give_back(1, lax.rem(me + groups // 2 + d, groups)).start()
        pl.when(d != groups // 2)(lambda: give_back(0, lax.rem(me + groups // 2 + d, groups)).start())
        return carry

    lax.fori_loop(0, groups, start_back, 0)
    keep = pltpu.make_async_copy(bsend.at[0, me], out_hbm.at[core * groups + me], isem.at[0])
    keep.start()

    sent = send.at[:, pl.ds(0, (groups - 1) * piece)]
    pltpu.make_async_copy(sent, sent, sa).wait()
    pltpu.make_async_copy(xbuf.at[:, 0], xbuf.at[:, 0], sx).wait()
    pltpu.make_async_copy(v_ref.at[0], v_ref.at[0], sf).wait()
    pltpu.make_async_copy(u_ref.at[0], u_ref.at[0], sf).wait()
    pltpu.make_async_copy(owner.at[0], owner.at[0], sf).wait()
    arrived = out_hbm.at[pl.ds(0, 2 * groups - 1)]
    keep.wait()
    pltpu.make_async_copy(arrived, arrived, sb).wait()
    pltpu.make_async_copy(arrived, arrived, rb).wait()


def series_kernel(band_ref, table_ref, out_hbm, wide, out, sem):
    q_low, q_high, sources, samples = out.shape
    block = band_ref.shape[0] // 2
    half = sources // 2
    low = band_ref[:block, :].astype(jnp.float32)
    high = band_ref[block:, :].astype(jnp.float32)
    first = lax.broadcasted_iota(jnp.int32, low.shape, 1) % sources < half
    wide[0] = jnp.where(first, low, pltpu.roll(high, half, 1))
    wide[1] = jnp.where(first, pltpu.roll(low, LANES - half, 1), high)

    for q in range(q_high):
        rows = pl.ds(q, block // q_high, stride=q_high)
        left = jnp.concatenate([wide[0, rows, :], wide[1, rows, :]], axis=0).T
        left = left.reshape(q_low, 2, 2, half // 2, left.shape[1])
        left = jnp.swapaxes(left, 1, 2).reshape(q_low * sources, left.shape[-1])
        series = jnp.dot(
            left.astype(jnp.bfloat16), table_ref[...], preferred_element_type=jnp.float32
        )
        out[:, q] = series.astype(jnp.bfloat16).reshape(q_low, sources, samples)
        pltpu.make_async_copy(out.at[:, q], out_hbm.at[:, q], sem).start()
    pltpu.make_async_copy(out, out_hbm, sem).wait()


def fast_device(wavefield, u_factors, v_factors, tile_ranks, tile_offsets):
    rec_dev, src_dev, samples = wavefield.shape
    freq_dev, tile, slots = u_factors.shape[1], u_factors.shape[3], u_factors.shape[4]
    groups = lax.axis_size("freq")
    chunks = rec_dev // tile
    steps, width = 2 * chunks, tile // 2
    freqs = freq_dev * groups
    forward, inverse = host_tables(freqs, samples)
    table = jnp.asarray(np.repeat(forward.T, src_dev, axis=1)).astype(jnp.bfloat16)
    inverse = inverse.reshape(freqs, 2, samples).transpose(1, 0, 2).reshape(2 * freqs, samples)
    inverse = jnp.asarray(inverse).astype(jnp.bfloat16)
    columns = table.shape[1]
    piece = columns // groups
    sources = 4 * src_dev
    q_dev = tile // groups
    q_low = LANES // sources
    q_high = q_dev // q_low
    band_rows = freq_dev * q_high
    factors = 2 * freq_dev
    vmem = pl.BlockSpec(memory_space=pltpu.VMEM)
    hbm = pl.BlockSpec(memory_space=pl.ANY)
    dma = pltpu.SemaphoreType.DMA
    bands = pl.pallas_call(
        functools.partial(band_kernel, groups, chunks, tile, src_dev),
        out_shape=jax.ShapeDtypeStruct((2 * groups, band_rows, LANES), jnp.bfloat16),
        in_specs=[hbm] * 6,
        out_specs=hbm,
        scratch_shapes=[
            pltpu.SMEM(tile_offsets[:, 0].shape, jnp.int32),
            pltpu.SMEM(tile_ranks[:, 0].shape, jnp.int32),
            pltpu.VMEM((samples, columns), jnp.bfloat16),
            pltpu.VMEM((2, factors, tile, slots), jnp.bfloat16),
            pltpu.VMEM((2, factors, slots, tile), jnp.bfloat16),
            pltpu.VMEM((2, freq_dev, 8, slots), jnp.int32),
            pltpu.VMEM((steps, width * src_dev, samples), jnp.bfloat16),
            pltpu.VMEM((columns // LANES, width * src_dev, LANES), jnp.float32),
            pltpu.VMEM((steps, columns, width), jnp.bfloat16),
            pltpu.VMEM((steps, 2, groups, piece, width), jnp.bfloat16),
            pltpu.VMEM((2, freq_dev, 2, 2, 2 * src_dev, slots), jnp.float32),
            pltpu.VMEM((2, groups, band_rows, LANES), jnp.bfloat16),
            dma((2,)), dma, dma, dma, dma((steps,)),
            dma, dma((steps, 3)), dma, dma((steps,)),
            dma, dma, dma, dma, dma, dma,
        ],
        compiler_params=pltpu.CompilerParams(
            collective_id=0, has_side_effects=True, vmem_limit_bytes=60 * 1024 * 1024
        ),
        name="bands",
    )(
        wavefield.reshape(rec_dev * src_dev, samples),
        table,
        u_factors.reshape(factors, tile, slots),
        v_factors.reshape(factors, slots, tile),
        tile_offsets[:, 0],
        tile_ranks[:, 0],
    ).reshape(2 * groups * band_rows, LANES)
    shape = (q_low, q_high, sources, samples)
    series = pl.pallas_call(
        series_kernel,
        out_shape=jax.ShapeDtypeStruct(shape, jnp.bfloat16),
        in_specs=[vmem, vmem],
        out_specs=hbm,
        scratch_shapes=[
            pltpu.VMEM((2, bands.shape[0] // 2, LANES), jnp.float32),
            pltpu.VMEM(shape, jnp.bfloat16),
            dma,
        ],
        name="series",
    )(bands, inverse)
    return series.reshape(q_dev, sources, samples)


def per_device(wavefield, u_factors, v_factors, tile_ranks, tile_offsets):
    rec_dev, src_dev, samples = wavefield.shape
    tile, slots = u_factors.shape[3], u_factors.shape[4]
    groups = lax.axis_size("freq")
    aligned = tile % LANES == 0 and rec_dev % tile == 0 and slots % LANES == 0
    aligned = aligned and samples % LANES == 0
    counts = u_factors.shape[1] == 2 and u_factors.shape[2] == 1 and src_dev == 8
    counts = counts and lax.axis_size("rows") == 4 and groups % 2 == 0
    if aligned and counts and tile == groups * 32:
        return fast_device(wavefield, u_factors, v_factors, tile_ranks, tile_offsets)
    return general_device(wavefield, u_factors, v_factors, tile_ranks, tile_offsets)


def solution(mesh):
    placed = (
        P("freq", "rows", None),
        P(None, "freq", "rows", None, None),
        P(None, "freq", "rows", None, None),
        P("freq", "rows", None),
        P("freq", "rows", None),
    )
    return jax.shard_map(
        per_device,
        mesh=mesh,
        in_specs=placed,
        out_specs=P(("rows", "freq"), None, None),
        check_vma=False,
    )
```

```python
import functools
import math

import jax
import jax.numpy as jnp
import numpy as np
from jax import lax
from jax.experimental import pallas as pl
from jax.experimental.pallas import tpu as pltpu
from jax.sharding import PartitionSpec as P

RANK_MAX = 64
MESH = pl.DeviceIdType.MESH
LANES = 128
LAG = 3
DIRECT = 3
OLAG = 5


def spectral_tables(freq_count, sample_count):
    freq_bins = jnp.arange(freq_count, dtype=jnp.int32) + 1
    sample_index = jnp.arange(sample_count, dtype=jnp.int32)
    phase_int = freq_bins[:, None] * sample_index[None, :] % sample_count
    angles = phase_int.astype(jnp.float32) * (2.0 * math.pi / sample_count)
    cosine = jnp.cos(angles)
    minus_sine = -jnp.sin(angles)
    stacked = jnp.stack([cosine, minus_sine], axis=1)
    forward = (stacked / math.sqrt(sample_count)).astype(jnp.bfloat16)
    inverse = (stacked / math.sqrt(freq_count)).astype(jnp.bfloat16)
    return (forward, inverse)


def tile_windows(v_row, u_row, starts, rank_max):
    columns = starts.shape[0]
    slot_index = (starts[:, None] + jnp.arange(rank_max, dtype=jnp.int32)[None, :]).reshape(-1)
    v_padded = jnp.pad(v_row, ((0, 0), (0, rank_max), (0, 0)))
    u_padded = jnp.pad(u_row, ((0, 0), (0, 0), (0, rank_max)))
    v_win = jnp.take(v_padded, slot_index, axis=1).reshape(2, columns, rank_max, v_row.shape[2])
    u_win = jnp.take(u_padded, slot_index, axis=2).reshape(2, u_row.shape[1], columns, rank_max)
    return (v_win, u_win)


def slot_lookup(starts, counts, rank_max, slot_count):
    position = jnp.arange(slot_count, dtype=jnp.int32)
    started = starts[:, None, :] <= position[None, :, None]
    owner_tile = jnp.sum(started.astype(jnp.int32), axis=2) - 1
    first_slot = jnp.max(jnp.where(started, starts[:, None, :], 0), axis=2)
    within = position[None, :] - first_slot
    live_slot = position[None, :] < (starts[:, -1] + counts[:, -1])[:, None]
    flat_index = jnp.where(live_slot, owner_tile * rank_max + within, 0)
    return (flat_index, live_slot)


def take_slots(values, chosen):
    return jnp.take(values, chosen, axis=1)


def general_device(wavefield, u_factors, v_factors, tile_ranks, tile_offsets):
    rec_dev, src_dev, samples = wavefield.shape
    freq_dev = u_factors.shape[1]
    rows_dev = u_factors.shape[2]
    tile_size = u_factors.shape[3]
    slot_count = u_factors.shape[4]
    freq_group = lax.axis_size("freq")
    row_group = lax.axis_size("rows")
    freqs = freq_dev * freq_group
    receivers = rec_dev * freq_group
    columns = receivers // tile_size
    sources = src_dev * row_group
    forward, inverse = spectral_tables(freqs, samples)
    spectrum = jnp.einsum("kct,rst->kcrs", forward, wavefield, preferred_element_type=jnp.float32)
    spectrum = spectrum.astype(jnp.bfloat16).reshape(freqs, 2, rec_dev * src_dev)
    windows = jax.vmap(
        functools.partial(tile_windows, rank_max=RANK_MAX), in_axes=(1, 1, 0), out_axes=(1, 1)
    )
    rank_slots = jnp.arange(RANK_MAX, dtype=jnp.int32)
    tile_row = 0
    v_win, u_win = windows(
        v_factors[:, :, tile_row], u_factors[:, :, tile_row], tile_offsets[:, tile_row]
    )
    rank_mask = rank_slots[None, None, :] < tile_ranks[:, tile_row, :, None]
    flat_index, live_slot = slot_lookup(
        tile_offsets[:, tile_row], tile_ranks[:, tile_row], RANK_MAX, slot_count
    )
    prepared = [(v_win, u_win, rank_mask, flat_index, live_slot)]
    by_frequency = lax.all_to_all(spectrum, "freq", split_axis=0, concat_axis=2, tiled=True)
    portion = lax.all_gather(by_frequency[None], "rows", axis=0, tiled=True)
    blocks_in = portion.shape[0]
    spectra = portion.reshape(blocks_in, freq_dev, 2, columns, tile_size, src_dev)
    spectra = jnp.transpose(spectra, (1, 2, 3, 4, 0, 5)).reshape(
        freq_dev, 2, columns, tile_size, blocks_in * src_dev
    )
    tile_row = 0
    v_win, u_win, rank_mask, flat_index, live_slot = prepared[tile_row]
    quadrants = jnp.einsum(
        "afjmr,fbjrs->fabjms", v_win, spectra, preferred_element_type=jnp.float32
    )
    coeffs = jnp.stack(
        [quadrants[:, 0, 0] - quadrants[:, 1, 1], quadrants[:, 0, 1] + quadrants[:, 1, 0]], axis=1
    )
    coeffs = jnp.where(rank_mask[:, None, :, :, None], coeffs, 0.0).astype(jnp.bfloat16)
    stacked = coeffs.reshape(freq_dev, 2, columns * RANK_MAX, blocks_in * src_dev)
    packed = jax.vmap(take_slots)(stacked, flat_index)
    packed = jnp.where(live_slot[:, None, :, None], packed, jnp.zeros((), jnp.bfloat16))
    products = jnp.einsum(
        "afrk,fcks->facrs", u_factors[:, :, tile_row], packed, preferred_element_type=jnp.float32
    )
    results = [
        jnp.stack(
            [products[:, 0, 0] - products[:, 1, 1], products[:, 0, 1] + products[:, 1, 0]], axis=1
        )
    ]
    merged = jnp.stack(results, axis=2)
    bands = merged.astype(jnp.bfloat16).reshape(
        freq_dev, 2, rows_dev * tile_size, blocks_in, src_dev
    )
    bands = bands.reshape(freq_dev, 2, rows_dev * tile_size * sources)
    returned = lax.all_to_all(bands, "freq", split_axis=2, concat_axis=0, tiled=True)
    series = jnp.einsum("kcq,kct->qt", returned, inverse, preferred_element_type=jnp.float32)
    return series.astype(jnp.bfloat16).reshape(rows_dev * tile_size // freq_group, sources, samples)


def host_tables(freq_count, sample_count):
    freq_bins = np.arange(freq_count) + 1
    phase = freq_bins[:, None] * np.arange(sample_count)[None, :] % sample_count
    angles = phase * (2.0 * math.pi / sample_count)
    stacked = np.stack([np.cos(angles), -np.sin(angles)], axis=1)
    stacked = stacked.reshape(2 * freq_count, sample_count)
    forward = (stacked / math.sqrt(sample_count)).astype(np.float32)
    inverse = (stacked / math.sqrt(freq_count)).astype(np.float32)
    return forward, inverse


def band_kernel(
    groups, chunks, tile, src_dev,
    wave, table_hbm, u_hbm, v_hbm, starts_hbm, counts_hbm, out_hbm,
    starts, counts, table, u_ref, v_ref, owner, wbuf, spec, send, xbuf, acc, bsend,
    isem, tsem, usem, vsem, wsem, sa, ra, sx, rx, sf, rv, ru, ro, sb, rb,
):
    me = lax.axis_index("freq")
    row = lax.axis_index("rows")
    core = lax.rem(row, 2)
    side = row // 2
    across = lax.rem(row + 2, 4)
    partner = row + 1 - 2 * core
    half = groups // 2
    quarter = groups // 4
    own_half = me // half
    place = me // quarter
    edge = 1 + (place * place - 3 * place) // 2
    steps = 2 * chunks
    width = tile // 2
    freq_dev = owner.shape[1]
    slots = owner.shape[3]
    rows = 2 * src_dev
    outer_first = (1 - own_half) * 3 * quarter
    inner_first = (2 - own_half) * quarter
    factors = u_ref.shape[1]
    step_rows = width * src_dev

    def load(h):
        return pltpu.make_async_copy(
            wave.at[pl.ds(h * step_rows, step_rows)], wbuf.at[h], wsem.at[h]
        )

    load_table = pltpu.make_async_copy(table_hbm, table, tsem)
    load_v = pltpu.make_async_copy(v_hbm, v_ref.at[0], vsem)
    load_u = pltpu.make_async_copy(u_hbm, u_ref.at[0], usem)
    load_starts = pltpu.make_async_copy(starts_hbm, starts, isem.at[0])
    load_counts = pltpu.make_async_copy(counts_hbm, counts, isem.at[1])
    load(0).start()
    load_table.start()
    load_starts.start()
    load_counts.start()

    barrier = pltpu.get_barrier_semaphore()

    def greet(d, carry):
        peer = lax.rem(me + d, groups)
        pl.semaphore_signal(barrier, inc=1, device_id=(peer, row), device_id_type=MESH)
        pl.semaphore_signal(barrier, inc=1, device_id=(peer, partner), device_id_type=MESH)
        return carry

    lax.fori_loop(1, groups, greet, 0)
    for d in range(half):
        peer = own_half * half + lax.rem(me + d, half)
        pl.semaphore_signal(barrier, inc=1, device_id=(peer, across), device_id_type=MESH)
    pl.semaphore_signal(barrier, inc=1, device_id=(me, partner), device_id_type=MESH)

    def start_load(h, carry):
        load(h).start()
        return carry

    lax.fori_loop(1, steps, start_load, 0)
    load_v.start()
    load_u.start()

    load_starts.wait()
    load_counts.wait()
    slot = lax.broadcasted_iota(jnp.int32, (8, slots), 1)
    for k in range(freq_dev):
        tiles = groups * chunks

        def count_started(j, held):
            return held + (slot >= starts[k, j]).astype(jnp.int32)

        held = lax.fori_loop(0, tiles, count_started, jnp.full((8, slots), -1, jnp.int32), unroll=8)
        live = slot < starts[k, tiles - 1] + counts[k, tiles - 1]
        owner[0, k] = jnp.where(live, held, -1)
    acc[...] = jnp.zeros_like(acc)
    lane_mod = lax.rem(lax.broadcasted_iota(jnp.int32, (width, LANES), 1), src_dev)

    def exchange(h, peer, sender, r_sem):
        return pltpu.make_async_remote_copy(
            src_ref=send.at[h, peer],
            dst_ref=xbuf.at[h, side, sender],
            send_sem=sa,
            recv_sem=r_sem,
            device_id=(peer, row),
            device_id_type=MESH,
        )

    def cross(h, first, count, block):
        return pltpu.make_async_remote_copy(
            src_ref=xbuf.at[h, block, pl.ds(first, count)],
            dst_ref=xbuf.at[h, block, pl.ds(first, count)],
            send_sem=sx,
            recv_sem=rx.at[h // 2],
            device_id=(me, across),
            device_id_type=MESH,
        )

    def to_partner(src, dst, r_sem):
        return pltpu.make_async_remote_copy(
            src_ref=src,
            dst_ref=dst,
            send_sem=sf,
            recv_sem=r_sem,
            device_id=(me, partner),
            device_id_type=MESH,
        )

    def share_v(n):
        return to_partner(v_hbm.at[n], v_ref.at[1, n], rv)

    def share_u(n):
        return to_partner(u_hbm.at[n], u_ref.at[1, n], ru)

    share_owner = to_partner(owner.at[0], owner.at[1], ro)

    def transform(h):
        load(h).wait()
        values = lax.dot_general(
            wbuf[h], table[...], (((1,), (0,)), ((), ())),
            preferred_element_type=jnp.float32,
        )
        for p in range(spec.shape[0]):
            spec[p] = values[:, p * LANES : (p + 1) * LANES]
        for p in range(spec.shape[0]):
            picked = spec[p, pl.ds(0, width, stride=src_dev), :]
            for s in range(1, src_dev):
                picked = jnp.where(
                    lane_mod == s, spec[p, pl.ds(s, width, stride=src_dev), :], picked
                )
            turned = picked.T.astype(jnp.bfloat16).reshape(-1, freq_dev, rows, width)
            peers = slice(p * turned.shape[0], (p + 1) * turned.shape[0])
            send[h, peers] = turned
        xbuf[h, side, me] = send[h, me]

    def direct(h, peer):
        return pltpu.make_async_remote_copy(
            src_ref=send.at[h, peer],
            dst_ref=xbuf.at[h, side, me],
            send_sem=sx,
            recv_sem=rx.at[h // 2],
            device_id=(peer, across),
            device_id_type=MESH,
        )

    def distribute(h):
        cross(h, me, 1, side).start()
        near = [own_half * half + lax.rem(me + d, half) for d in range(1, half)]
        for peer in near:
            exchange(h, peer, me, ra.at[h, 0]).start()
        for d in range(half):
            peer = (1 - own_half) * half + lax.rem(me + d, half)
            exchange(h, peer, me, ra.at[h, 1 + edge]).start()
        pl.when(h < DIRECT)(lambda: [direct(h, peer).start() for peer in near] and None)

    def relay_near(h):
        pltpu.make_async_copy(
            xbuf.at[h, side, pl.ds(0, half - 1)], xbuf.at[h, side, pl.ds(0, half - 1)], ra.at[h, 0]
        ).wait()
        near = [own_half * half + lax.rem(me + d, half) for d in range(1, half)]
        pl.when(h >= DIRECT)(lambda: [cross(h, peer, 1, side).start() for peer in near] and None)

    def relay_far(h, outer):
        first = outer_first if outer else inner_first
        block = xbuf.at[h, side, pl.ds(first, quarter)]
        pltpu.make_async_copy(block, block, ra.at[h, 1 + outer]).wait()
        cross(h, first, quarter, side).start()

    def relay_inner(h):
        relay_far(h, 0)

    def relay_outer(h):
        relay_far(h, 1)

    def crossed(c):
        block = xbuf.at[pl.ds(0, 2), 1 - side]
        pltpu.make_async_copy(block, block, rx.at[c]).wait()

    def project(c):
        crossed(c)
        for k in range(freq_dev):
            halves = [xbuf[2 * c + n, :, :, k].reshape(2 * groups * rows, width) for n in range(2)]
            left = jnp.concatenate(halves, axis=1)
            for i in range(2):
                held = owner[i, k]
                inside = [(held == g * chunks + c)[None, None] for g in range(groups)]
                for a in range(2):
                    products = lax.dot_general(
                        left, v_ref[i, a * freq_dev + k], (((1,), (1,)), ((), ())),
                        preferred_element_type=jnp.float32,
                    ).reshape(2, groups, 2, src_dev, slots)
                    total = acc[i, k, a].reshape(2, 2, src_dev, slots)
                    for g in range(groups):
                        total = jnp.where(inside[g], products[:, g], total)
                    acc[i, k, a] = total.reshape(2, rows, slots)

    def first_pass(h, carry):
        transform(h)
        pl.when(h == 0)(lambda: pl.semaphore_wait(barrier, 2 * groups + half - 1))
        distribute(h)
        pl.when(h == 1)(share_owner.start)
        pl.when((h >= 2) & (h < 2 + factors))(lambda: share_v(h - 2).start())
        pl.when((h >= 2 + factors) & (h < 2 + 2 * factors))(lambda: share_u(h - 2 - factors).start())
        pl.when(h >= LAG)(lambda: relay_near(h - LAG))
        pl.when(h >= OLAG)(lambda: relay_outer(h - OLAG))
        pl.when((h > LAG + 1) & (lax.rem(h, 2) == 1))(lambda: relay_inner((h - LAG - 2) // 2))
        return carry

    load_table.wait()
    lax.fori_loop(0, steps, first_pass, 0)
    load_v.wait()
    to_partner(v_ref.at[0], v_ref.at[1], rv).wait_recv()
    share_owner.wait_recv()

    late = (steps - LAG - 1) // 2
    order = [("inner", late), ("near", steps - 3), ("outer", steps - 5), ("outer", steps - 4)]
    order += [("project", 0), ("outer", steps - 3), ("inner", late + 1), ("near", steps - 2)]
    order += [("outer", steps - 2), ("inner", late + 2), ("inner", late + 3), ("project", 1)]
    order += [("inner", late + 4), ("near", steps - 1), ("outer", steps - 1)]
    order += [("inner", h) for h in range(late + 5, steps)]
    order += [("project", c) for c in range(2, chunks)]
    turns, turn = [], []
    for kind, n in order:
        if kind == "project":
            turns.append(turn)
            turn = []
        else:
            turn.append((kind, n))
    relays = {"near": relay_near, "inner": relay_inner, "outer": relay_outer}

    def relay_turn(c):
        for n, turn in enumerate(turns):
            if turn:
                pl.when(c == n)(lambda turn=turn: [relays[kind](h) for kind, h in turn] and None)

    def second_pass(c, carry):
        relay_turn(c)
        project(c)
        return carry

    lax.fori_loop(0, chunks, second_pass, 0)

    load_u.wait()
    to_partner(u_ref.at[0], u_ref.at[1], ru).wait_recv()

    def give_back(i, peer):
        return pltpu.make_async_remote_copy(
            src_ref=bsend.at[i, peer],
            dst_ref=out_hbm.at[core * groups + me],
            send_sem=sb,
            recv_sem=rb,
            device_id=(peer, row + i * (partner - row)),
            device_id_type=MESH,
        )

    contract = (((1,), (1,)), ((), ()))
    q_low = LANES // (2 * rows)
    q_high = tile // groups // q_low
    for i in (core, 1 - core):
        for k in range(freq_dev):
            first = acc[i, k, 0].reshape(2, 2, src_dev, slots)
            second = acc[i, k, 1].reshape(2, 2, src_dev, slots)
            real = (first[:, 0] - second[:, 1]).reshape(rows, slots)
            imag = (first[:, 1] + second[:, 0]).reshape(rows, slots)
            straight = jnp.concatenate([real, imag], axis=0).astype(jnp.bfloat16)
            turned = jnp.concatenate([-imag, real], axis=0).astype(jnp.bfloat16)
            band = lax.dot_general(
                u_ref[i, k], straight, contract, preferred_element_type=jnp.float32
            )
            band = band + lax.dot_general(
                u_ref[i, freq_dev + k], turned, contract, preferred_element_type=jnp.float32
            )
            parts = band.reshape(groups, q_low, q_high, 2 * rows)
            parts = jnp.concatenate([parts[:, q] for q in range(q_low)], axis=-1)
            bsend[i, :, k] = parts.astype(jnp.bfloat16)

        def start_back(d, carry, i=i):
            peer = (1 - own_half) * (groups - 1) + (2 * own_half - 1) * d
            pl.when((i == 1) | (peer != me))(lambda: give_back(i, peer).start())
            return carry

        lax.fori_loop(0, groups, start_back, 0)
    keep = pltpu.make_async_copy(bsend.at[0, me], out_hbm.at[core * groups + me], isem.at[0])
    keep.start()

    sent = send.at[:, pl.ds(0, groups - 1)]
    pltpu.make_async_copy(sent, sent, sa).wait()
    pltpu.make_async_copy(xbuf.at[:, 0], xbuf.at[:, 0], sx).wait()
    pltpu.make_async_copy(v_ref.at[0], v_ref.at[0], sf).wait()
    pltpu.make_async_copy(u_ref.at[0], u_ref.at[0], sf).wait()
    pltpu.make_async_copy(owner.at[0], owner.at[0], sf).wait()
    keep.wait()
    back = out_hbm.at[pl.ds(0, 2 * groups - 1)]
    pltpu.make_async_copy(back, back, sb).wait()
    pltpu.make_async_copy(back, back, rb).wait()


def series_kernel(band_ref, table_ref, out_hbm, wide, out, sem):
    q_low, q_high, sources, samples = out.shape
    block = band_ref.shape[0] // 2
    half = sources // 2
    low = band_ref[:block, :].astype(jnp.float32)
    high = band_ref[block:, :].astype(jnp.float32)
    first = lax.broadcasted_iota(jnp.int32, low.shape, 1) % sources < half
    wide[0] = jnp.where(first, low, pltpu.roll(high, half, 1))
    wide[1] = jnp.where(first, pltpu.roll(low, LANES - half, 1), high)

    for q in range(q_high):
        rows = pl.ds(q, block // q_high, stride=q_high)
        left = jnp.concatenate([wide[0, rows, :], wide[1, rows, :]], axis=0).T
        left = left.reshape(q_low, 2, 2, half // 2, left.shape[1])
        left = jnp.swapaxes(left, 1, 2).reshape(q_low * sources, left.shape[-1])
        series = jnp.dot(
            left.astype(jnp.bfloat16), table_ref[...], preferred_element_type=jnp.float32
        )
        out[:, q] = series.astype(jnp.bfloat16).reshape(q_low, sources, samples)
        pltpu.make_async_copy(out.at[:, q], out_hbm.at[:, q], sem).start()
    pltpu.make_async_copy(out, out_hbm, sem).wait()


def fast_device(wavefield, u_factors, v_factors, tile_ranks, tile_offsets):
    rec_dev, src_dev, samples = wavefield.shape
    freq_dev, tile, slots = u_factors.shape[1], u_factors.shape[3], u_factors.shape[4]
    groups = lax.axis_size("freq")
    chunks = rec_dev // tile
    steps, width = 2 * chunks, tile // 2
    freqs = freq_dev * groups
    forward, inverse = host_tables(freqs, samples)
    table = jnp.asarray(np.repeat(forward.T, src_dev, axis=1)).astype(jnp.bfloat16)
    inverse = inverse.reshape(freqs, 2, samples).transpose(1, 0, 2).reshape(2 * freqs, samples)
    inverse = jnp.asarray(inverse).astype(jnp.bfloat16)
    columns = table.shape[1]
    sources = 4 * src_dev
    q_dev = tile // groups
    q_low = LANES // sources
    q_high = q_dev // q_low
    factors = 2 * freq_dev
    vmem = pl.BlockSpec(memory_space=pltpu.VMEM)
    hbm = pl.BlockSpec(memory_space=pl.ANY)
    dma = pltpu.SemaphoreType.DMA
    bands = pl.pallas_call(
        functools.partial(band_kernel, groups, chunks, tile, src_dev),
        out_shape=jax.ShapeDtypeStruct((2 * groups, freq_dev, q_high, LANES), jnp.bfloat16),
        in_specs=[hbm] * 6,
        out_specs=hbm,
        scratch_shapes=[
            pltpu.SMEM(tile_offsets[:, 0].shape, jnp.int32),
            pltpu.SMEM(tile_ranks[:, 0].shape, jnp.int32),
            pltpu.VMEM((samples, columns), jnp.bfloat16),
            pltpu.VMEM((2, factors, tile, slots), jnp.bfloat16),
            pltpu.VMEM((2, factors, slots, tile), jnp.bfloat16),
            pltpu.VMEM((2, freq_dev, 8, slots), jnp.int32),
            pltpu.VMEM((steps, width * src_dev, samples), jnp.bfloat16),
            pltpu.VMEM((columns // LANES, width * src_dev, LANES), jnp.float32),
            pltpu.VMEM((steps, groups, freq_dev, 2 * src_dev, width), jnp.bfloat16),
            pltpu.VMEM((steps, 2, groups, freq_dev, 2 * src_dev, width), jnp.bfloat16),
            pltpu.VMEM((2, freq_dev, 2, 2, 2 * src_dev, slots), jnp.float32),
            pltpu.VMEM((2, groups, freq_dev, q_high, LANES), jnp.bfloat16),
            dma((2,)), dma, dma, dma, dma((steps,)),
            dma, dma((steps, 3)), dma, dma((chunks,)),
            dma, dma, dma, dma, dma, dma,
        ],
        compiler_params=pltpu.CompilerParams(
            collective_id=0, has_side_effects=True, vmem_limit_bytes=60 * 1024 * 1024
        ),
        name="bands",
    )(
        wavefield.reshape(rec_dev * src_dev, samples),
        table,
        u_factors.reshape(factors, tile, slots),
        v_factors.reshape(factors, slots, tile),
        tile_offsets[:, 0],
        tile_ranks[:, 0],
    ).reshape(2 * groups * freq_dev * q_high, LANES)
    shape = (q_low, q_high, sources, samples)
    series = pl.pallas_call(
        series_kernel,
        out_shape=jax.ShapeDtypeStruct(shape, jnp.bfloat16),
        in_specs=[vmem, vmem],
        out_specs=hbm,
        scratch_shapes=[
            pltpu.VMEM((2, bands.shape[0] // 2, LANES), jnp.float32),
            pltpu.VMEM(shape, jnp.bfloat16),
            dma,
        ],
        name="series",
    )(bands, inverse)
    return series.reshape(q_dev, sources, samples)


def per_device(wavefield, u_factors, v_factors, tile_ranks, tile_offsets):
    rec_dev, src_dev, samples = wavefield.shape
    tile, slots = u_factors.shape[3], u_factors.shape[4]
    groups = lax.axis_size("freq")
    aligned = tile % LANES == 0 and rec_dev % tile == 0 and slots % LANES == 0
    aligned = aligned and samples % LANES == 0
    counts = u_factors.shape[1] == 2 and u_factors.shape[2] == 1 and src_dev == 8
    counts = counts and lax.axis_size("rows") == 4 and groups % 2 == 0
    if aligned and counts and tile == groups * 32 and rec_dev >= 4 * tile:
        return fast_device(wavefield, u_factors, v_factors, tile_ranks, tile_offsets)
    return general_device(wavefield, u_factors, v_factors, tile_ranks, tile_offsets)


def solution(mesh):
    placed = (
        P("freq", "rows", None),
        P(None, "freq", "rows", None, None),
        P(None, "freq", "rows", None, None),
        P("freq", "rows", None),
        P("freq", "rows", None),
    )
    return jax.shard_map(
        per_device,
        mesh=mesh,
        in_specs=placed,
        out_specs=P(("rows", "freq"), None, None),
        check_vma=False,
    )
```

```python
import functools
import math

import jax
import jax.numpy as jnp
import numpy as np
from jax import lax
from jax.experimental import pallas as pl
from jax.experimental.pallas import tpu as pltpu
from jax.sharding import PartitionSpec as P

RANK_MAX = 64
MESH = pl.DeviceIdType.MESH
LANES = 128
LAG = 3
DIRECT = 3
OLAG = 5


def spectral_tables(freq_count, sample_count):
    freq_bins = jnp.arange(freq_count, dtype=jnp.int32) + 1
    sample_index = jnp.arange(sample_count, dtype=jnp.int32)
    phase_int = freq_bins[:, None] * sample_index[None, :] % sample_count
    angles = phase_int.astype(jnp.float32) * (2.0 * math.pi / sample_count)
    cosine = jnp.cos(angles)
    minus_sine = -jnp.sin(angles)
    stacked = jnp.stack([cosine, minus_sine], axis=1)
    forward = (stacked / math.sqrt(sample_count)).astype(jnp.bfloat16)
    inverse = (stacked / math.sqrt(freq_count)).astype(jnp.bfloat16)
    return (forward, inverse)


def tile_windows(v_row, u_row, starts, rank_max):
    columns = starts.shape[0]
    slot_index = (starts[:, None] + jnp.arange(rank_max, dtype=jnp.int32)[None, :]).reshape(-1)
    v_padded = jnp.pad(v_row, ((0, 0), (0, rank_max), (0, 0)))
    u_padded = jnp.pad(u_row, ((0, 0), (0, 0), (0, rank_max)))
    v_win = jnp.take(v_padded, slot_index, axis=1).reshape(2, columns, rank_max, v_row.shape[2])
    u_win = jnp.take(u_padded, slot_index, axis=2).reshape(2, u_row.shape[1], columns, rank_max)
    return (v_win, u_win)


def slot_lookup(starts, counts, rank_max, slot_count):
    position = jnp.arange(slot_count, dtype=jnp.int32)
    started = starts[:, None, :] <= position[None, :, None]
    owner_tile = jnp.sum(started.astype(jnp.int32), axis=2) - 1
    first_slot = jnp.max(jnp.where(started, starts[:, None, :], 0), axis=2)
    within = position[None, :] - first_slot
    live_slot = position[None, :] < (starts[:, -1] + counts[:, -1])[:, None]
    flat_index = jnp.where(live_slot, owner_tile * rank_max + within, 0)
    return (flat_index, live_slot)


def take_slots(values, chosen):
    return jnp.take(values, chosen, axis=1)


def general_device(wavefield, u_factors, v_factors, tile_ranks, tile_offsets):
    rec_dev, src_dev, samples = wavefield.shape
    freq_dev = u_factors.shape[1]
    rows_dev = u_factors.shape[2]
    tile_size = u_factors.shape[3]
    slot_count = u_factors.shape[4]
    freq_group = lax.axis_size("freq")
    row_group = lax.axis_size("rows")
    freqs = freq_dev * freq_group
    receivers = rec_dev * freq_group
    columns = receivers // tile_size
    sources = src_dev * row_group
    forward, inverse = spectral_tables(freqs, samples)
    spectrum = jnp.einsum("kct,rst->kcrs", forward, wavefield, preferred_element_type=jnp.float32)
    spectrum = spectrum.astype(jnp.bfloat16).reshape(freqs, 2, rec_dev * src_dev)
    windows = jax.vmap(
        functools.partial(tile_windows, rank_max=RANK_MAX), in_axes=(1, 1, 0), out_axes=(1, 1)
    )
    rank_slots = jnp.arange(RANK_MAX, dtype=jnp.int32)
    tile_row = 0
    v_win, u_win = windows(
        v_factors[:, :, tile_row], u_factors[:, :, tile_row], tile_offsets[:, tile_row]
    )
    rank_mask = rank_slots[None, None, :] < tile_ranks[:, tile_row, :, None]
    flat_index, live_slot = slot_lookup(
        tile_offsets[:, tile_row], tile_ranks[:, tile_row], RANK_MAX, slot_count
    )
    prepared = [(v_win, u_win, rank_mask, flat_index, live_slot)]
    by_frequency = lax.all_to_all(spectrum, "freq", split_axis=0, concat_axis=2, tiled=True)
    portion = lax.all_gather(by_frequency[None], "rows", axis=0, tiled=True)
    blocks_in = portion.shape[0]
    spectra = portion.reshape(blocks_in, freq_dev, 2, columns, tile_size, src_dev)
    spectra = jnp.transpose(spectra, (1, 2, 3, 4, 0, 5)).reshape(
        freq_dev, 2, columns, tile_size, blocks_in * src_dev
    )
    tile_row = 0
    v_win, u_win, rank_mask, flat_index, live_slot = prepared[tile_row]
    quadrants = jnp.einsum(
        "afjmr,fbjrs->fabjms", v_win, spectra, preferred_element_type=jnp.float32
    )
    coeffs = jnp.stack(
        [quadrants[:, 0, 0] - quadrants[:, 1, 1], quadrants[:, 0, 1] + quadrants[:, 1, 0]], axis=1
    )
    coeffs = jnp.where(rank_mask[:, None, :, :, None], coeffs, 0.0).astype(jnp.bfloat16)
    stacked = coeffs.reshape(freq_dev, 2, columns * RANK_MAX, blocks_in * src_dev)
    packed = jax.vmap(take_slots)(stacked, flat_index)
    packed = jnp.where(live_slot[:, None, :, None], packed, jnp.zeros((), jnp.bfloat16))
    products = jnp.einsum(
        "afrk,fcks->facrs", u_factors[:, :, tile_row], packed, preferred_element_type=jnp.float32
    )
    results = [
        jnp.stack(
            [products[:, 0, 0] - products[:, 1, 1], products[:, 0, 1] + products[:, 1, 0]], axis=1
        )
    ]
    merged = jnp.stack(results, axis=2)
    bands = merged.astype(jnp.bfloat16).reshape(
        freq_dev, 2, rows_dev * tile_size, blocks_in, src_dev
    )
    bands = bands.reshape(freq_dev, 2, rows_dev * tile_size * sources)
    returned = lax.all_to_all(bands, "freq", split_axis=2, concat_axis=0, tiled=True)
    series = jnp.einsum("kcq,kct->qt", returned, inverse, preferred_element_type=jnp.float32)
    return series.astype(jnp.bfloat16).reshape(rows_dev * tile_size // freq_group, sources, samples)


def host_tables(freq_count, sample_count):
    freq_bins = np.arange(freq_count) + 1
    phase = freq_bins[:, None] * np.arange(sample_count)[None, :] % sample_count
    angles = phase * (2.0 * math.pi / sample_count)
    stacked = np.stack([np.cos(angles), -np.sin(angles)], axis=1)
    stacked = stacked.reshape(2 * freq_count, sample_count)
    forward = (stacked / math.sqrt(sample_count)).astype(np.float32)
    inverse = (stacked / math.sqrt(freq_count)).astype(np.float32)
    return forward, inverse


def band_kernel(
    groups, chunks, tile, src_dev,
    wave, table_hbm, u_hbm, v_hbm, starts_hbm, counts_hbm, out_hbm,
    starts, counts, table, u_ref, v_ref, owner, wbuf, spec, send, xbuf, acc, bsend,
    isem, tsem, usem, vsem, wsem, sa, ra, sx, rx, sf, rv, ru, ro, sb, rb,
):
    me = lax.axis_index("freq")
    row = lax.axis_index("rows")
    core = lax.rem(row, 2)
    side = row // 2
    across = lax.rem(row + 2, 4)
    partner = row + 1 - 2 * core
    half = groups // 2
    quarter = groups // 4
    own_half = me // half
    place = me // quarter
    edge = 1 + (place * place - 3 * place) // 2
    steps = 2 * chunks
    width = tile // 2
    freq_dev = owner.shape[1]
    slots = owner.shape[3]
    rows = 2 * src_dev
    outer_first = (1 - own_half) * 3 * quarter
    inner_first = (2 - own_half) * quarter
    factors = u_ref.shape[1]
    step_rows = width * src_dev

    def load(c):
        return pltpu.make_async_copy(
            wave.at[pl.ds(2 * c, 2)], wbuf.at[pl.ds(2 * c, 2)], wsem.at[c + 1]
        )

    def load_first(h):
        return pltpu.make_async_copy(wave.at[h], wbuf.at[h], wsem.at[h])

    load_table = pltpu.make_async_copy(table_hbm, table, tsem)
    load_v = pltpu.make_async_copy(v_hbm, v_ref.at[0], vsem)
    load_u = pltpu.make_async_copy(u_hbm, u_ref.at[0], usem)
    load_starts = pltpu.make_async_copy(starts_hbm, starts, isem.at[0])
    load_counts = pltpu.make_async_copy(counts_hbm, counts, isem.at[1])
    load_first(0).start()
    load_table.start()
    load_first(1).start()
    load_starts.start()
    load_counts.start()

    barrier = pltpu.get_barrier_semaphore()

    def greet(d, carry):
        peer = lax.rem(me + d, groups)
        pl.semaphore_signal(barrier, inc=1, device_id=(peer, row), device_id_type=MESH)
        pl.semaphore_signal(barrier, inc=1, device_id=(peer, partner), device_id_type=MESH)
        return carry

    lax.fori_loop(1, groups, greet, 0)
    for d in range(half):
        peer = own_half * half + lax.rem(me + d, half)
        pl.semaphore_signal(barrier, inc=1, device_id=(peer, across), device_id_type=MESH)
    pl.semaphore_signal(barrier, inc=1, device_id=(me, partner), device_id_type=MESH)

    def start_load(h, carry):
        load(h).start()
        return carry

    lax.fori_loop(1, chunks, start_load, 0)
    load_v.start()
    load_u.start()

    load_starts.wait()
    load_counts.wait()
    slot = lax.broadcasted_iota(jnp.int32, (8, slots), 1)
    for k in range(freq_dev):
        tiles = groups * chunks

        def count_started(j, held):
            return held + (slot >= starts[k, j]).astype(jnp.int32)

        held = lax.fori_loop(0, tiles, count_started, jnp.full((8, slots), -1, jnp.int32), unroll=8)
        live = slot < starts[k, tiles - 1] + counts[k, tiles - 1]
        owner[0, k] = jnp.where(live, held, -1)
    acc[...] = jnp.zeros_like(acc)
    lane_mod = lax.rem(lax.broadcasted_iota(jnp.int32, (width, LANES), 1), src_dev)

    def exchange(h, peer, sender, r_sem):
        return pltpu.make_async_remote_copy(
            src_ref=send.at[h, peer],
            dst_ref=xbuf.at[h, side, sender],
            send_sem=sa,
            recv_sem=r_sem,
            device_id=(peer, row),
            device_id_type=MESH,
        )

    def cross(h, first, count, block):
        return pltpu.make_async_remote_copy(
            src_ref=xbuf.at[h, block, pl.ds(first, count)],
            dst_ref=xbuf.at[h, block, pl.ds(first, count)],
            send_sem=sx,
            recv_sem=rx.at[h // 2],
            device_id=(me, across),
            device_id_type=MESH,
        )

    def to_partner(src, dst, r_sem):
        return pltpu.make_async_remote_copy(
            src_ref=src,
            dst_ref=dst,
            send_sem=sf,
            recv_sem=r_sem,
            device_id=(me, partner),
            device_id_type=MESH,
        )

    def share_v(n):
        return to_partner(v_hbm.at[n], v_ref.at[1, n], rv)

    def share_u(n):
        return to_partner(u_hbm.at[n], u_ref.at[1, n], ru)

    share_owner = to_partner(owner.at[0], owner.at[1], ro)

    def transform(h):
        pl.when(h < 2)(lambda: load_first(h).wait())
        pl.when((h > 1) & (lax.rem(h, 2) == 0))(lambda: load(h // 2).wait())
        values = lax.dot_general(
            wbuf[h], table[...], (((1,), (0,)), ((), ())),
            preferred_element_type=jnp.float32,
        )
        for p in range(spec.shape[0]):
            spec[p] = values[:, p * LANES : (p + 1) * LANES]
        for p in range(spec.shape[0]):
            picked = spec[p, pl.ds(0, width, stride=src_dev), :]
            for s in range(1, src_dev):
                picked = jnp.where(
                    lane_mod == s, spec[p, pl.ds(s, width, stride=src_dev), :], picked
                )
            turned = picked.T.astype(jnp.bfloat16).reshape(-1, freq_dev, rows, width)
            peers = slice(p * turned.shape[0], (p + 1) * turned.shape[0])
            send[h, peers] = turned
        xbuf[h, side, me] = send[h, me]

    def direct(h, peer):
        return pltpu.make_async_remote_copy(
            src_ref=send.at[h, peer],
            dst_ref=xbuf.at[h, side, me],
            send_sem=sx,
            recv_sem=rx.at[h // 2],
            device_id=(peer, across),
            device_id_type=MESH,
        )

    def distribute(h):
        cross(h, me, 1, side).start()
        near = [own_half * half + lax.rem(me + d, half) for d in range(1, half)]
        for peer in near:
            exchange(h, peer, me, ra.at[h, 0]).start()
        for d in range(half):
            peer = (1 - own_half) * half + lax.rem(me + d, half)
            exchange(h, peer, me, ra.at[h, 1 + edge]).start()
        pl.when(h < DIRECT)(lambda: [direct(h, peer).start() for peer in near] and None)

    def relay_near(h):
        pltpu.make_async_copy(
            xbuf.at[h, side, pl.ds(0, half - 1)], xbuf.at[h, side, pl.ds(0, half - 1)], ra.at[h, 0]
        ).wait()
        near = [own_half * half + lax.rem(me + d, half) for d in range(1, half)]
        pl.when(h >= DIRECT)(lambda: [cross(h, peer, 1, side).start() for peer in near] and None)

    def relay_far(h, outer):
        first = outer_first if outer else inner_first
        block = xbuf.at[h, side, pl.ds(first, quarter)]
        pltpu.make_async_copy(block, block, ra.at[h, 1 + outer]).wait()
        cross(h, first, quarter, side).start()

    def relay_inner(h):
        relay_far(h, 0)

    def relay_outer(h):
        relay_far(h, 1)

    def crossed(c):
        block = xbuf.at[pl.ds(0, 2), 1 - side]
        pltpu.make_async_copy(block, block, rx.at[c]).wait()

    def project(c):
        crossed(c)
        for k in range(freq_dev):
            halves = [xbuf[2 * c + n, :, :, k].reshape(2 * groups * rows, width) for n in range(2)]
            left = jnp.concatenate(halves, axis=1)
            for i in range(2):
                held = owner[i, k]
                inside = [(held == g * chunks + c)[None, None] for g in range(groups)]
                for a in range(2):
                    products = lax.dot_general(
                        left, v_ref[i, a * freq_dev + k], (((1,), (1,)), ((), ())),
                        preferred_element_type=jnp.float32,
                    ).reshape(2, groups, 2, src_dev, slots)
                    total = acc[i, k, a].reshape(2, 2, src_dev, slots)
                    for g in range(groups):
                        total = jnp.where(inside[g], products[:, g], total)
                    acc[i, k, a] = total.reshape(2, rows, slots)

    def first_pass(h, carry):
        transform(h)
        pl.when(h == 0)(lambda: pl.semaphore_wait(barrier, 2 * groups + half - 1))
        distribute(h)
        pl.when(h == 1)(share_owner.start)
        pl.when((h >= 2) & (h < 2 + factors))(lambda: share_v(h - 2).start())
        pl.when((h >= 2 + factors) & (h < 2 + 2 * factors))(lambda: share_u(h - 2 - factors).start())
        pl.when(h >= LAG)(lambda: relay_near(h - LAG))
        pl.when(h >= OLAG)(lambda: relay_outer(h - OLAG))
        pl.when((h > LAG + 1) & (lax.rem(h, 2) == 1))(lambda: relay_inner((h - LAG - 2) // 2))
        return carry

    load_table.wait()
    lax.fori_loop(0, steps, first_pass, 0)
    load_v.wait()
    to_partner(v_ref.at[0], v_ref.at[1], rv).wait_recv()
    share_owner.wait_recv()

    late = (steps - LAG - 1) // 2
    order = [("inner", late), ("near", steps - 3), ("outer", steps - 5), ("outer", steps - 4)]
    order += [("project", 0), ("outer", steps - 3), ("inner", late + 1), ("near", steps - 2)]
    order += [("outer", steps - 2), ("inner", late + 2), ("inner", late + 3), ("project", 1)]
    order += [("inner", late + 4), ("near", steps - 1), ("outer", steps - 1)]
    order += [("inner", h) for h in range(late + 5, steps)]
    order += [("project", c) for c in range(2, chunks)]
    turns, turn = [], []
    for kind, n in order:
        if kind == "project":
            turns.append(turn)
            turn = []
        else:
            turn.append((kind, n))
    relays = {"near": relay_near, "inner": relay_inner, "outer": relay_outer}

    def relay_turn(c):
        for n, turn in enumerate(turns):
            if turn:
                pl.when(c == n)(lambda turn=turn: [relays[kind](h) for kind, h in turn] and None)

    def second_pass(c, carry):
        relay_turn(c)
        project(c)
        return carry

    lax.fori_loop(0, chunks, second_pass, 0)

    load_u.wait()
    to_partner(u_ref.at[0], u_ref.at[1], ru).wait_recv()

    def give_back(i, peer):
        return pltpu.make_async_remote_copy(
            src_ref=bsend.at[i, peer],
            dst_ref=out_hbm.at[core * groups + me],
            send_sem=sb,
            recv_sem=rb,
            device_id=(peer, row + i * (partner - row)),
            device_id_type=MESH,
        )

    contract = (((1,), (1,)), ((), ()))
    q_low = LANES // (2 * rows)
    q_high = tile // groups // q_low
    for i in (core, 1 - core):
        for k in range(freq_dev):
            first = acc[i, k, 0].reshape(2, 2, src_dev, slots)
            second = acc[i, k, 1].reshape(2, 2, src_dev, slots)
            real = (first[:, 0] - second[:, 1]).reshape(rows, slots)
            imag = (first[:, 1] + second[:, 0]).reshape(rows, slots)
            straight = jnp.concatenate([real, imag], axis=0).astype(jnp.bfloat16)
            turned = jnp.concatenate([-imag, real], axis=0).astype(jnp.bfloat16)
            band = lax.dot_general(
                u_ref[i, k], straight, contract, preferred_element_type=jnp.float32
            )
            band = band + lax.dot_general(
                u_ref[i, freq_dev + k], turned, contract, preferred_element_type=jnp.float32
            )
            parts = band.reshape(groups, q_low, q_high, 2 * rows)
            parts = jnp.concatenate([parts[:, q] for q in range(q_low)], axis=-1)
            bsend[i, :, k] = parts.astype(jnp.bfloat16)

        def start_back(d, carry, i=i):
            peer = (1 - own_half) * (groups - 1) + (2 * own_half - 1) * d
            pl.when((i == 1) | (peer != me))(lambda: give_back(i, peer).start())
            return carry

        lax.fori_loop(0, groups, start_back, 0)
    keep = pltpu.make_async_copy(bsend.at[0, me], out_hbm.at[core * groups + me], isem.at[0])
    keep.start()

    sent = send.at[:, pl.ds(0, groups - 1)]
    pltpu.make_async_copy(sent, sent, sa).wait()
    pltpu.make_async_copy(xbuf.at[:, 0], xbuf.at[:, 0], sx).wait()
    pltpu.make_async_copy(v_ref.at[0], v_ref.at[0], sf).wait()
    pltpu.make_async_copy(u_ref.at[0], u_ref.at[0], sf).wait()
    pltpu.make_async_copy(owner.at[0], owner.at[0], sf).wait()
    keep.wait()
    back = out_hbm.at[pl.ds(0, 2 * groups - 1)]
    pltpu.make_async_copy(back, back, sb).wait()
    pltpu.make_async_copy(back, back, rb).wait()


def series_kernel(band_ref, table_ref, out_hbm, wide, out, sem):
    q_low, q_high, sources, samples = out.shape
    block = band_ref.shape[0] // 2
    half = sources // 2
    low = band_ref[:block, :].astype(jnp.float32)
    high = band_ref[block:, :].astype(jnp.float32)
    first = lax.broadcasted_iota(jnp.int32, low.shape, 1) % sources < half
    wide[0] = jnp.where(first, low, pltpu.roll(high, half, 1))
    wide[1] = jnp.where(first, pltpu.roll(low, LANES - half, 1), high)

    for q in range(q_high):
        rows = pl.ds(q, block // q_high, stride=q_high)
        left = jnp.concatenate([wide[0, rows, :], wide[1, rows, :]], axis=0).T
        left = left.reshape(q_low, 2, 2, half // 2, left.shape[1])
        left = jnp.swapaxes(left, 1, 2).reshape(q_low * sources, left.shape[-1])
        series = jnp.dot(
            left.astype(jnp.bfloat16), table_ref[...], preferred_element_type=jnp.float32
        )
        out[:, q] = series.astype(jnp.bfloat16).reshape(q_low, sources, samples)
        pltpu.make_async_copy(out.at[:, q], out_hbm.at[:, q], sem).start()
    pltpu.make_async_copy(out, out_hbm, sem).wait()


def fast_device(wavefield, u_factors, v_factors, tile_ranks, tile_offsets):
    rec_dev, src_dev, samples = wavefield.shape
    freq_dev, tile, slots = u_factors.shape[1], u_factors.shape[3], u_factors.shape[4]
    groups = lax.axis_size("freq")
    chunks = rec_dev // tile
    steps, width = 2 * chunks, tile // 2
    freqs = freq_dev * groups
    forward, inverse = host_tables(freqs, samples)
    table = jnp.asarray(np.repeat(forward.T, src_dev, axis=1)).astype(jnp.bfloat16)
    inverse = inverse.reshape(freqs, 2, samples).transpose(1, 0, 2).reshape(2 * freqs, samples)
    inverse = jnp.asarray(inverse).astype(jnp.bfloat16)
    columns = table.shape[1]
    sources = 4 * src_dev
    q_dev = tile // groups
    q_low = LANES // sources
    q_high = q_dev // q_low
    factors = 2 * freq_dev
    vmem = pl.BlockSpec(memory_space=pltpu.VMEM)
    hbm = pl.BlockSpec(memory_space=pl.ANY)
    dma = pltpu.SemaphoreType.DMA
    bands = pl.pallas_call(
        functools.partial(band_kernel, groups, chunks, tile, src_dev),
        out_shape=jax.ShapeDtypeStruct((2 * groups, freq_dev, q_high, LANES), jnp.bfloat16),
        in_specs=[hbm] * 6,
        out_specs=hbm,
        scratch_shapes=[
            pltpu.SMEM(tile_offsets[:, 0].shape, jnp.int32),
            pltpu.SMEM(tile_ranks[:, 0].shape, jnp.int32),
            pltpu.VMEM((samples, columns), jnp.bfloat16),
            pltpu.VMEM((2, factors, tile, slots), jnp.bfloat16),
            pltpu.VMEM((2, factors, slots, tile), jnp.bfloat16),
            pltpu.VMEM((2, freq_dev, 8, slots), jnp.int32),
            pltpu.VMEM((steps, width * src_dev, samples), jnp.bfloat16),
            pltpu.VMEM((columns // LANES, width * src_dev, LANES), jnp.float32),
            pltpu.VMEM((steps, groups, freq_dev, 2 * src_dev, width), jnp.bfloat16),
            pltpu.VMEM((steps, 2, groups, freq_dev, 2 * src_dev, width), jnp.bfloat16),
            pltpu.VMEM((2, freq_dev, 2, 2, 2 * src_dev, slots), jnp.float32),
            pltpu.VMEM((2, groups, freq_dev, q_high, LANES), jnp.bfloat16),
            dma((2,)), dma, dma, dma, dma((chunks + 1,)),
            dma, dma((steps, 3)), dma, dma((chunks,)),
            dma, dma, dma, dma, dma, dma,
        ],
        compiler_params=pltpu.CompilerParams(
            collective_id=0, has_side_effects=True, vmem_limit_bytes=60 * 1024 * 1024
        ),
        name="bands",
    )(
        wavefield.reshape(steps, width * src_dev, samples),
        table,
        u_factors.reshape(factors, tile, slots),
        v_factors.reshape(factors, slots, tile),
        tile_offsets[:, 0],
        tile_ranks[:, 0],
    ).reshape(2 * groups * freq_dev * q_high, LANES)
    shape = (q_low, q_high, sources, samples)
    series = pl.pallas_call(
        series_kernel,
        out_shape=jax.ShapeDtypeStruct(shape, jnp.bfloat16),
        in_specs=[vmem, vmem],
        out_specs=hbm,
        scratch_shapes=[
            pltpu.VMEM((2, bands.shape[0] // 2, LANES), jnp.float32),
            pltpu.VMEM(shape, jnp.bfloat16),
            dma,
        ],
        name="series",
    )(bands, inverse)
    return series.reshape(q_dev, sources, samples)


def per_device(wavefield, u_factors, v_factors, tile_ranks, tile_offsets):
    rec_dev, src_dev, samples = wavefield.shape
    tile, slots = u_factors.shape[3], u_factors.shape[4]
    groups = lax.axis_size("freq")
    aligned = tile % LANES == 0 and rec_dev % tile == 0 and slots % LANES == 0
    aligned = aligned and samples % LANES == 0
    counts = u_factors.shape[1] == 2 and u_factors.shape[2] == 1 and src_dev == 8
    counts = counts and lax.axis_size("rows") == 4 and groups % 2 == 0
    if aligned and counts and tile == groups * 32 and rec_dev >= 4 * tile:
        return fast_device(wavefield, u_factors, v_factors, tile_ranks, tile_offsets)
    return general_device(wavefield, u_factors, v_factors, tile_ranks, tile_offsets)


def solution(mesh):
    placed = (
        P("freq", "rows", None),
        P(None, "freq", "rows", None, None),
        P(None, "freq", "rows", None, None),
        P("freq", "rows", None),
        P("freq", "rows", None),
    )
    return jax.shard_map(
        per_device,
        mesh=mesh,
        in_specs=placed,
        out_specs=P(("rows", "freq"), None, None),
        check_vma=False,
    )
```
